128 devices in a mesh: stage: 2 (over core), data: 64 (over z, y, x).
Axes of the slice: x: 4, y: 4, z: 4, core: 2. Of those that a mesh axis runs over, the one named last changes fastest.
Arguments:
- inputs: bfloat16 [512, 64, 1024], P('data')
- targets: bfloat16 [512, 64, 1024], P('data')
- w_up: bfloat16 [4, 1024, 4096], P('stage')
- w_down: bfloat16 [4, 4096, 1024], P('stage')
Outputs:
- output 1: float32 [], replicated
- output 2: float32 [4, 1024, 4096], P('stage', 'data')
- output 3: float32 [4, 4096, 1024], P('stage', None, 'data')
All inputs are finite; a program needn't handle non-finite values.
Results may differ from the reference program's by a relative error of at most 0.00239958.
Values are sent between devices in bfloat16 or wider.
A program may use at most 1 GiB of HBM per device.

```python
import jax
import jax.numpy as jnp
from jax import lax

WIDTH = 1024
FFN = 4096
TOKENS = 64
MICRO = 8
REPLICAS = 64
LAYERS = 4

BATCH = REPLICAS * MICRO
TOTAL_TOKENS = BATCH * TOKENS


def setup_inputs(seed: int = 0) -> dict:
    base_key = jax.random.key(seed)
    key_in, key_tgt, key_up, key_down = jax.random.split(base_key, 4)
    inputs = jax.random.normal(key_in, (BATCH, TOKENS, WIDTH), jnp.float32).astype(jnp.bfloat16)
    targets = jax.random.normal(key_tgt, (BATCH, TOKENS, WIDTH), jnp.float32).astype(jnp.bfloat16)
    up_scale = WIDTH ** -0.5
    down_scale = 1.5 * (FFN * LAYERS) ** -0.5
    w_up = (jax.random.normal(key_up, (LAYERS, WIDTH, FFN), jnp.float32) * up_scale).astype(jnp.bfloat16)
    w_down = (jax.random.normal(key_down, (LAYERS, FFN, WIDTH), jnp.float32) * down_scale).astype(jnp.bfloat16)
    return {'inputs': inputs, 'targets': targets, 'w_up': w_up, 'w_down': w_down}


def layer_forward(h_in, w_one, w_two):
    pre_act = jnp.dot(h_in, w_one, preferred_element_type=jnp.float32).astype(jnp.bfloat16)
    act_out = jax.nn.gelu(pre_act.astype(jnp.float32)).astype(jnp.bfloat16)
    branch = jnp.dot(act_out, w_two, preferred_element_type=jnp.float32)
    return (h_in.astype(jnp.float32) + branch).astype(jnp.bfloat16)


def backward_inputs(h_in, grad_out, w_one, w_two):
    pre_act = jnp.dot(h_in, w_one, preferred_element_type=jnp.float32).astype(jnp.bfloat16)
    pre_wide = pre_act.astype(jnp.float32)
    act_out = jax.nn.gelu(pre_wide).astype(jnp.bfloat16)
    grad_act = jnp.dot(grad_out, w_two.T, preferred_element_type=jnp.float32).astype(jnp.bfloat16)
    grad_pre = jax.jvp(jax.nn.gelu, (pre_wide,), (grad_act.astype(jnp.float32),))[1].astype(jnp.bfloat16)
    grad_in = (grad_out.astype(jnp.float32) + jnp.dot(grad_pre, w_one.T, preferred_element_type=jnp.float32)).astype(jnp.bfloat16)
    return grad_in, act_out, grad_pre


def backward_weights(h_in, act_out, grad_pre, grad_out):
    grad_one = jnp.dot(h_in.T, grad_pre, preferred_element_type=jnp.float32)
    grad_two = jnp.dot(act_out.T, grad_out, preferred_element_type=jnp.float32)
    return grad_one, grad_two


def reference(inputs, targets, w_up, w_down):
    def fwd_step(hidden, weights):
        return layer_forward(hidden, weights[0], weights[1]), hidden

    def bwd_step(grad_out, layer_in):
        h_in, w_one, w_two = layer_in
        grad_in, act_out, grad_pre = backward_inputs(h_in, grad_out, w_one, w_two)
        return grad_in, backward_weights(h_in, act_out, grad_pre, grad_out)

    def micro_step(loop_state, batch_pair):
        up_acc, down_acc, loss_acc = loop_state
        x_mb, y_mb = batch_pair
        h_top, h_saved = lax.scan(fwd_step, x_mb, (w_up, w_down))
        out_diff = h_top.astype(jnp.float32) - y_mb.astype(jnp.float32)
        loss_mb = jnp.sum(out_diff * out_diff) / (2 * TOTAL_TOKENS)
        top_grad = (out_diff / TOTAL_TOKENS).astype(jnp.bfloat16)
        layer_grads = lax.scan(bwd_step, top_grad, (h_saved, w_up, w_down), reverse=True)[1]
        return (up_acc + layer_grads[0], down_acc + layer_grads[1], loss_acc + loss_mb), None

    init_state = (jnp.zeros(w_up.shape, jnp.float32), jnp.zeros(w_down.shape, jnp.float32), jnp.zeros((), jnp.float32))
    final_state = lax.scan(micro_step, init_state, (inputs, targets))[0]
    return final_state[2], final_state[0], final_state[1]
```

```python
import functools

import jax
import jax.numpy as jnp
from jax import lax
from jax.experimental import pallas as pl
from jax.experimental.pallas import tpu as pltpu
from jax.sharding import PartitionSpec as P

CONTRACT_LAST = (((1,), (1,)), ((), ()))
CONTRACT_FIRST = (((0,), (0,)), ((), ()))
MESH = pl.DeviceIdType.MESH
RING = 4
STRIDE = {'x': 1, 'y': 4, 'z': 16}
GROUP_AXIS = ('x', 'y')
COLS = 256
N_CHUNKS = 16
STREAMS = (
    (0, 'y', 'z', 0, 6),
    (1, 'x', 'z', 8, 6),
    (0, 'z', 'y', 6, 2),
    (1, 'z', 'x', 14, 2),
)


def position(data_idx, axis):
    return lax.rem(lax.div(data_idx, STRIDE[axis]), RING)


def neighbour(data_idx, axis, shift):
    here = position(data_idx, axis)
    return data_idx + (lax.rem(here + shift, RING) - here) * STRIDE[axis]


def meet(stage_idx, data_idx, peers):
    barrier = pltpu.get_barrier_semaphore()
    for axis, shift in peers:
        pl.semaphore_signal(barrier, inc=1, device_id=(stage_idx, neighbour(data_idx, axis, shift)), device_id_type=MESH)
    pl.semaphore_wait(barrier, len(peers))


def gather_kernel(h0, e0, h1, e1, loss_in, gh0, ge0, gh1, ge1, loss_out, loss_acc, loss_recv,
                  send_sem, recv_sem, own_sem, loss_send, loss_got):
    stage_idx = lax.axis_index('stage')
    data_idx = lax.axis_index('data')
    meet(stage_idx, data_idx, [(axis, shift) for axis in 'xyz' for shift in (1, 2, 3)])

    def remote(src, dst, axis, shift, send, recv):
        return pltpu.make_async_remote_copy(
            src_ref=src, dst_ref=dst, send_sem=send, recv_sem=recv,
            device_id=(stage_idx, neighbour(data_idx, axis, shift)), device_id_type=MESH)

    def loss_copies(phase):
        axis = 'xyz'[phase]
        return [remote(loss_acc.at[phase], loss_recv.at[phase, shift - 1], axis, shift,
                       loss_send.at[phase, shift - 1], loss_got.at[phase, shift - 1]) for shift in (1, 2, 3)]

    def loss_finish(phase):
        for copy in loss_copies(phase):
            copy.wait()
        total = loss_acc[phase]
        for idx in range(3):
            total = total + loss_recv[phase, idx]
        return total

    loss_acc[0] = loss_in[...]
    for copy in loss_copies(0):
        copy.start()
    groups = ((h0, e0, gh0, ge0), (h1, e1, gh1, ge1))
    pending = []
    locals_ = []
    relays = []
    for slot, (h_ref, e_ref, gh, ge) in enumerate(groups):
        axis = GROUP_AXIS[slot]
        here = position(data_idx, axis)
        for kind, (src, dst) in enumerate(((h_ref, gh), (e_ref, ge))):
            copy = pltpu.make_async_copy(src, dst.at[here], own_sem.at[slot, kind])
            copy.start()
            locals_.append(copy)
        for order in range(2):
            for side, shift in ((0, 1), (1, 3)):
                src, dst = ((h_ref, gh), (e_ref, ge))[order ^ side]
                copy = remote(src, dst.at[here], axis, shift, send_sem.at[slot, side, order], recv_sem.at[slot, side, order])
                copy.start()
                pending.append((slot, side, order, copy))
        for side, shift, buf in ((0, 1, gh), (1, 3, ge)):
            origin = lax.rem(here + RING - shift, RING)
            relays.append((slot, side, remote(buf.at[origin], buf.at[origin], axis, shift,
                                              send_sem.at[slot, side, 2], recv_sem.at[slot, side, 2])))
    loss_acc[1] = loss_finish(0)
    for copy in loss_copies(1):
        copy.start()
    first = {(slot, side): copy for slot, side, order, copy in pending if order == 0}
    for slot, side, relay in relays:
        first[(slot, side)].wait_recv()
        relay.start()
    loss_acc[2] = loss_finish(1)
    for copy in loss_copies(2):
        copy.start()
    loss_out[...] = loss_finish(2)
    for copy in locals_:
        copy.wait()
    for slot, side, order, copy in pending:
        if order == 0:
            copy.wait_send()
        else:
            copy.wait()
    for slot, side, relay in relays:
        relay.wait()


def gather_groups(h0, e0, h1, e1, loss_part):
    full = jax.ShapeDtypeStruct((RING,) + h0.shape, h0.dtype)
    vmem = pl.BlockSpec(memory_space=pltpu.VMEM)
    hbm = pl.BlockSpec(memory_space=pl.ANY)
    return pl.pallas_call(
        gather_kernel,
        out_shape=(full, full, full, full, jax.ShapeDtypeStruct(loss_part.shape, jnp.float32)),
        in_specs=[vmem] * 5,
        out_specs=(hbm, hbm, hbm, hbm, vmem),
        scratch_shapes=[
            pltpu.VMEM((3,) + loss_part.shape, jnp.float32),
            pltpu.VMEM((3, 3) + loss_part.shape, jnp.float32),
            pltpu.SemaphoreType.DMA((2, 2, 3)),
            pltpu.SemaphoreType.DMA((2, 2, 3)),
            pltpu.SemaphoreType.DMA((2, 2)),
            pltpu.SemaphoreType.DMA((3, 3)),
            pltpu.SemaphoreType.DMA((3, 3)),
        ],
        compiler_params=pltpu.CompilerParams(collective_id=0, has_side_effects=True),
        name='gather_groups',
    )(h0, e0, h1, e1, loss_part)


def scatter_kernel(up0, dn0, up1, dn1, out, part, r1, r2, r3, r4, final,
                   load_sem, s1_send, s1_recv, s2_send, s2_recv, s3_send, s3_recv, s4_send, s4_recv, a_send, a_recv):
    stage_idx = lax.axis_index('stage')
    data_idx = lax.axis_index('data')
    pos = {axis: position(data_idx, axis) for axis in 'xyz'}
    sources = (up0, dn0, up1, dn1)
    loads = [pltpu.make_async_copy(
        sources[chunk // 4].at[:, :, :, :, pl.ds((chunk % 4) * COLS, COLS)], part.at[chunk], load_sem.at[chunk])
        for chunk in range(N_CHUNKS)]
    n_waves = max(stream[4] for stream in STREAMS)
    for wave in range(n_waves):
        for stream in STREAMS:
            if wave < stream[4]:
                loads[stream[3] + wave].start()
    meet(stage_idx, data_idx, [(axis, shift) for axis in 'xyz' for shift in ((1, 3) if axis == 'z' else (1, 2, 3))])

    low, high, every = pl.ds(0, 2), pl.ds(2, 2), pl.ds(0, 4)

    def shifted(axis, shift):
        return lax.rem(pos[axis] + shift, RING)

    def remote(src, dst, axis, shift, send, recv):
        return pltpu.make_async_remote_copy(
            src_ref=src, dst_ref=dst, send_sem=send, recv_sem=recv,
            device_id=(stage_idx, neighbour(data_idx, axis, shift)), device_id_type=MESH)

    def where_of(chunk, sel):
        return (chunk,) + tuple(sel[axis] for axis in 'zyx')

    def add_into(chunk, sel, buf, prefix, lead):
        free = [axis for axis in 'zyx' if axis in lead]
        counts = [lead[axis][1] for axis in free]
        for flat in range(counts[0] * (counts[1] if len(counts) > 1 else 1)):
            idx = (flat,) if len(counts) == 1 else (flat // counts[1], flat % counts[1])
            point = dict(sel)
            for axis, value in zip(free, idx):
                point[axis] = lead[axis][0] + value
            dst = where_of(chunk, point)
            src = prefix[:-1] + (prefix[-1] + idx[0],) + idx[1:]
            part[dst] = part[dst] + buf[src]

    class Stream:
        def __init__(self, spec):
            self.slot, self.first, self.second, self.base, self.count = spec
            self.rest = GROUP_AXIS[self.slot]
            free = [axis for axis in 'zyx' if axis != self.first]
            self.split, self.other = free

        def phase_copies(self, chunk, phase, kind):
            axis = (self.first, self.second)[phase]
            wide, narrow = ((r1, r2), (r3, r4))[phase]
            send, recv = (((s1_send, s1_recv), (s2_send, s2_recv)), ((s3_send, s3_recv), (s4_send, s4_recv)))[phase][kind == 2]
            copies = []
            for side in range(2):
                half = (low, high)[side ^ (kind == 1)]
                to_axis = shifted(axis, 2 if kind == 0 else (1, 3)[side])
                if phase == 0:
                    sel = {axis: to_axis, self.split: half, self.other: every}
                else:
                    sel = {self.first: pos[self.first], axis: to_axis, self.rest: half}
                dst = narrow.at[chunk, side] if kind == 2 else wide.at[chunk, side, (low, high)[kind]]
                sem_idx = (chunk, side) if kind == 2 else (chunk, side, kind)
                copies.append(remote(part.at[where_of(chunk, sel)], dst, axis, (1, 3)[side], send.at[sem_idx], recv.at[sem_idx]))
            return copies

        def exchange(self, chunk):
            g = self.rest
            copies = []
            for shift in (1, 2, 3):
                sel = {self.first: pos[self.first], self.second: pos[self.second], g: shifted(g, shift)}
                copies.append(remote(part.at[where_of(chunk, sel)], final.at[chunk, pos[g]], g, shift,
                                     a_send.at[chunk, shift - 1], a_recv.at[chunk, shift - 1]))
            return copies

        def run(self, step, chunk):
            a, b, g = self.first, self.second, self.rest
            if step == 0:
                pltpu.make_async_copy(up0.at[:, :, :, :, pl.ds(0, COLS)], part.at[chunk], load_sem.at[chunk]).wait()
                for kind in (0, 1):
                    for copy in self.phase_copies(chunk, 0, kind):
                        copy.start()
            elif step == 1:
                relay, direct, combined = [self.phase_copies(chunk, 0, kind) for kind in range(3)]
                span = {self.other: (0, 4)}
                for side, (shift, start) in enumerate(((1, 0), (3, 2))):
                    relay[side].wait_recv()
                    add_into(chunk, {a: shifted(a, shift)}, r1, (chunk, side, 0), {self.split: (start, 2), **span})
                    combined[side].start()
                for side, start in ((0, 2), (1, 0)):
                    direct[side].wait_recv()
                    add_into(chunk, {a: pos[a]}, r1, (chunk, side, 2), {self.split: (start, 2), **span})
            elif step == 2:
                combined = self.phase_copies(chunk, 0, 2)
                for side, start in ((0, 0), (1, 2)):
                    combined[side].wait_recv()
                    add_into(chunk, {a: pos[a]}, r2, (chunk, side, 0), {self.split: (start, 2), self.other: (0, 4)})
                for kind in (0, 1):
                    for copy in self.phase_copies(chunk, 1, kind):
                        copy.start()
            elif step == 3:
                relay, direct, combined = [self.phase_copies(chunk, 1, kind) for kind in range(3)]
                for side, (shift, start) in enumerate(((1, 0), (3, 2))):
                    relay[side].wait_recv()
                    add_into(chunk, {a: pos[a], b: shifted(b, shift)}, r3, (chunk, side, 0), {g: (start, 2)})
                    combined[side].start()
                for side, start in ((0, 2), (1, 0)):
                    direct[side].wait_recv()
                    add_into(chunk, {a: pos[a], b: pos[b]}, r3, (chunk, side, 2), {g: (start, 2)})
            elif step == 4:
                combined = self.phase_copies(chunk, 1, 2)
                for side, start in ((0, 0), (1, 2)):
                    combined[side].wait_recv()
                    add_into(chunk, {a: pos[a], b: pos[b]}, r4, (chunk, side, 0), {g: (start, 2)})
                for copy in self.exchange(chunk):
                    copy.start()
                final[chunk, pos[g]] = part[where_of(chunk, {a: pos[a], b: pos[b], g: pos[g]})]
            else:
                for copy in self.exchange(chunk):
                    copy.wait()
                for phase in range(2):
                    for kind in range(3):
                        for copy in self.phase_copies(chunk, phase, kind):
                            copy.wait_send()

    streams = [Stream(spec) for spec in STREAMS]

    def wave_body(wave, carry):
        for step in range(6):
            for stream in streams:
                item = wave - step

                @pl.when(jnp.logical_and(item >= 0, item < stream.count))
                def _():
                    stream.run(step, stream.base + item)
        return carry

    lax.fori_loop(0, n_waves + 5, wave_body, 0)
    out[...] = final[...]


def scatter_sums(up0, dn0, up1, dn1):
    n_rows, n_cols = up0.shape
    block = n_rows // (RING * RING * RING)
    views = [arr.reshape(RING, RING, RING, block, n_cols) for arr in (up0, dn0, up1, dn1)]
    f32 = jnp.float32
    dma = pltpu.SemaphoreType.DMA
    return pl.pallas_call(
        scatter_kernel,
        out_shape=jax.ShapeDtypeStruct((N_CHUNKS, RING, block, COLS), f32),
        in_specs=[pl.BlockSpec(memory_space=pl.ANY)] * 4,
        out_specs=pl.BlockSpec(memory_space=pltpu.VMEM),
        scratch_shapes=[
            pltpu.VMEM((N_CHUNKS, RING, RING, RING, block, COLS), f32),
            pltpu.VMEM((N_CHUNKS, 2, 4, 4, block, COLS), f32),
            pltpu.VMEM((N_CHUNKS, 2, 2, 4, block, COLS), f32),
            pltpu.VMEM((N_CHUNKS, 2, 4, block, COLS), f32),
            pltpu.VMEM((N_CHUNKS, 2, 2, block, COLS), f32),
            pltpu.VMEM((N_CHUNKS, RING, block, COLS), f32),
            dma((N_CHUNKS,)),
            dma((N_CHUNKS, 2, 2)), dma((N_CHUNKS, 2, 2)),
            dma((N_CHUNKS, 2)), dma((N_CHUNKS, 2)),
            dma((N_CHUNKS, 2, 2)), dma((N_CHUNKS, 2, 2)),
            dma((N_CHUNKS, 2)), dma((N_CHUNKS, 2)),
            dma((N_CHUNKS, 3)), dma((N_CHUNKS, 3)),
        ],
        compiler_params=pltpu.CompilerParams(collective_id=1, has_side_effects=True, vmem_limit_bytes=48 * 1024 * 1024),
        name='scatter_sums',
    )(*views)


def layer_forward(h_in, w_one, w_two):
    pre_act = jnp.dot(h_in, w_one, preferred_element_type=jnp.float32).astype(jnp.bfloat16)
    act_out = jax.nn.gelu(pre_act.astype(jnp.float32)).astype(jnp.bfloat16)
    branch = jnp.dot(act_out, w_two, preferred_element_type=jnp.float32)
    return (h_in.astype(jnp.float32) + branch).astype(jnp.bfloat16), pre_act


def hidden_grad(pre_act, grad_out, w_two):
    grad_act = lax.dot_general(grad_out, w_two, CONTRACT_LAST, preferred_element_type=jnp.float32).astype(jnp.bfloat16)
    pre_wide = pre_act.astype(jnp.float32)
    return jax.jvp(jax.nn.gelu, (pre_wide,), (grad_act.astype(jnp.float32),))[1].astype(jnp.bfloat16)


def layer_backward(pre_act, grad_out, w_one, w_two):
    grad_pre = hidden_grad(pre_act, grad_out, w_two)
    back_sum = lax.dot_general(grad_pre, w_one, CONTRACT_LAST, preferred_element_type=jnp.float32)
    return (grad_out.astype(jnp.float32) + back_sum).astype(jnp.bfloat16)


def block_weight_grads(h_all, e_all, w_one, w_two, pos, n_cols):
    n_width = h_all.shape[-1]
    h_all = h_all.reshape(-1, n_width)
    e_all = e_all.reshape(-1, n_width)
    one = lax.dynamic_slice(w_one, (0, pos * n_cols), (n_width, n_cols))
    two = lax.dynamic_slice(w_two, (pos * n_cols, 0), (n_cols, n_width))
    pre_act = jnp.dot(h_all, one, preferred_element_type=jnp.float32).astype(jnp.bfloat16)
    act_out = jax.nn.gelu(pre_act.astype(jnp.float32)).astype(jnp.bfloat16)
    grad_pre = hidden_grad(pre_act, e_all, two)
    grad_one = lax.dot_general(h_all, grad_pre, CONTRACT_FIRST, preferred_element_type=jnp.float32)
    grad_two = lax.dot_general(e_all, act_out, CONTRACT_FIRST, preferred_element_type=jnp.float32)
    return grad_one, grad_two


def solution(mesh):
    replicas = mesh.shape['data']

    def per_device(x_loc, y_loc, w_up, w_down):
        n_micro, n_tokens, n_width = x_loc.shape
        n_ffn = w_up.shape[2]
        total_tokens = replicas * n_micro * n_tokens
        stage_idx = lax.axis_index('stage')
        data_idx = lax.axis_index('data')
        x_all = x_loc.reshape(n_micro * n_tokens, n_width)
        y_all = y_loc.reshape(n_micro * n_tokens, n_width)

        def forward(h_in):
            h_mid, pre0 = layer_forward(h_in, w_up[0], w_down[0])
            h_out, pre1 = layer_forward(h_mid, w_up[1], w_down[1])
            return h_mid, h_out, pre0, pre1

        h_mid, h_out, _, pre1 = forward(x_all)
        h_recv = lax.ppermute(h_out, 'stage', [(0, 1)])

        def upper(_):
            h_mid, h_out, pre0, pre1 = forward(h_recv)
            diff = h_out.astype(jnp.float32) - y_all.astype(jnp.float32)
            loss = jnp.sum(diff * diff) / (2 * total_tokens)
            e_top = (diff / total_tokens).astype(jnp.bfloat16)
            e_mid = layer_backward(pre1, e_top, w_up[1], w_down[1])
            e_low = layer_backward(pre0, e_mid, w_up[0], w_down[0])
            return h_recv, h_mid, e_mid, e_top, e_low, jnp.full((8, 128), loss, jnp.float32)

        def lower(_):
            return x_all, h_mid, x_all, x_all, x_all, jnp.zeros((8, 128), jnp.float32)

        h0, h1, e0, e1, e_low, loss_part = lax.cond(stage_idx == 1, upper, lower, 0)
        e_recv = lax.ppermute(e_low, 'stage', [(1, 0)])
        loss_recv = lax.ppermute(loss_part, 'stage', [(1, 0)])
        loss_part = loss_part + loss_recv

        e0, e1 = lax.cond(
            stage_idx == 0,
            lambda _: (layer_backward(pre1, e_recv, w_up[1], w_down[1]), e_recv),
            lambda _: (e0, e1), 0)

        gh0, ge0, gh1, ge1, loss_sum = gather_groups(h0, e0, h1, e1, loss_part)
        n_cols = n_ffn // RING
        up0, dn0 = block_weight_grads(gh0, ge0, w_up[0], w_down[0], position(data_idx, GROUP_AXIS[0]), n_cols)
        up1, dn1 = block_weight_grads(gh1, ge1, w_up[1], w_down[1], position(data_idx, GROUP_AXIS[1]), n_cols)
        sums = scatter_sums(up0, dn0, up1, dn1)
        block = sums.shape[2]
        sums = sums.reshape(2, 2, n_cols // COLS, RING, block, COLS)
        grad_up = sums[:, 0].transpose(0, 3, 2, 1, 4).reshape(2, block, n_ffn)
        grad_down = sums[:, 1].transpose(0, 2, 1, 4, 3).reshape(2, n_ffn, block)
        return loss_sum[0, 0], grad_up, grad_down

    return jax.shard_map(
        per_device,
        mesh=mesh,
        in_specs=(P('data', None, None), P('data', None, None), P('stage', None, None), P('stage', None, None)),
        out_specs=(P(), P('stage', 'data', None), P('stage', None, 'data')),
        check_vma=False,
    )
```

```python
import functools

import jax
import jax.numpy as jnp
from jax import lax
from jax.experimental import pallas as pl
from jax.experimental.pallas import tpu as pltpu
from jax.sharding import PartitionSpec as P

CONTRACT_LAST = (((1,), (1,)), ((), ()))
CONTRACT_FIRST = (((0,), (0,)), ((), ()))
MESH = pl.DeviceIdType.MESH
RING = 4
STRIDE = {'x': 1, 'y': 4, 'z': 16}
GROUP_AXIS = ('x', 'y')
COLS = 256
HIDDEN = 512
N_CHUNKS = 16
ROOT = (2.0 / 3.141592653589793) ** 0.5
CUBIC = 0.044715


WAVES = ((1, 0), (1, 1), (0, 0), (0, 1))
OUTER = ('y', 'x')


def position(data_idx, axis):
    return lax.rem(lax.div(data_idx, STRIDE[axis]), RING)


def neighbour(data_idx, axis, shift):
    here = position(data_idx, axis)
    return data_idx + (lax.rem(here + shift, RING) - here) * STRIDE[axis]


def meet(stage_idx, data_idx, peers):
    barrier = pltpu.get_barrier_semaphore()
    for axis, shift in peers:
        pl.semaphore_signal(barrier, inc=1, device_id=(stage_idx, neighbour(data_idx, axis, shift)), device_id_type=MESH)
    pl.semaphore_wait(barrier, len(peers))


def gelu_parts(x):
    square = x * x
    tanh = jnp.tanh(x * (ROOT + (ROOT * CUBIC) * square))
    cdf = 0.5 + 0.5 * tanh
    slope = cdf + (0.5 * x) * ((1.0 - tanh * tanh) * (ROOT + (3.0 * ROOT * CUBIC) * square))
    return x * cdf, slope


def weight_kernel(gh0, gh1, ge1, e0, w_one, w_two, loss_in, out, loss_out,
                  gh, ge, one, two, act, grad, part, r1, r2, r3, r4, loss_acc, loss_recv,
                  gh_sem, ge_sem, one_sem, two_sem, e_send, e_recv,
                  s1_send, s1_recv, s2_send, s2_recv, s3_send, s3_recv, s4_send, s4_recv, a_send, a_recv,
                  loss_send, loss_got):
    stage_idx = lax.axis_index('stage')
    data_idx = lax.axis_index('data')
    pos = {axis: position(data_idx, axis) for axis in 'xyz'}
    n_rows = gh.shape[2]
    n_cols = w_one.shape[2] // RING

    def remote(src, dst, axis, shift, send, recv):
        return pltpu.make_async_remote_copy(
            src_ref=src, dst_ref=dst, send_sem=send, recv_sem=recv,
            device_id=(stage_idx, neighbour(data_idx, axis, shift)), device_id_type=MESH)

    def weight_copies(wave):
        slot, half = WAVES[wave]
        span = pl.ds(pl.multiple_of(pos[GROUP_AXIS[slot]] * n_cols + half * HIDDEN, HIDDEN), HIDDEN)
        return (
            pltpu.make_async_copy(w_one.at[slot, :, span], one.at[wave % 2], one_sem.at[wave]),
            pltpu.make_async_copy(w_two.at[slot, span, :], two.at[wave % 2], two_sem.at[wave]),
        )

    own_e = pltpu.make_async_copy(e0, ge.at[0, pos['x']], ge_sem.at[0])
    own_e.start()
    fills = {1: [pltpu.make_async_copy(gh1, gh.at[1], gh_sem.at[1]), pltpu.make_async_copy(ge1, ge.at[1], ge_sem.at[1])],
             0: [pltpu.make_async_copy(gh0, gh.at[0], gh_sem.at[0])]}
    for copy in fills[1] + list(weight_copies(0)) + fills[0] + list(weight_copies(1)):
        copy.start()
    meet(stage_idx, data_idx, [(axis, shift) for axis in 'xyz' for shift in (1, 2, 3)])

    here = pos['x']
    rows = (pl.ds(0, n_rows // 2), pl.ds(n_rows // 2, n_rows // 2))
    own_e.wait()
    directs = [remote(ge.at[0, here], ge.at[0, here], 'x', (1, 3)[side], e_send.at[side], e_recv.at[side]) for side in range(2)]
    for copy in directs:
        copy.start()

    def e_relays():
        copies = []
        for side, shift in ((0, 1), (1, 3)):
            block = ge.at[0, lax.rem(here + RING - shift, RING), rows[side]]
            copies.append(remote(block, block, 'x', shift, e_send.at[2 + side], e_recv.at[2 + side]))
        return copies

    def loss_copies(phase):
        return [remote(loss_acc.at[phase], loss_recv.at[phase, shift - 1], 'xyz'[phase], shift,
                       loss_send.at[phase, shift - 1], loss_got.at[phase, shift - 1]) for shift in (1, 2, 3)]

    def loss_start(phase):
        for copy in loss_copies(phase):
            copy.start()

    def loss_finish(phase):
        for copy in loss_copies(phase):
            copy.wait()
        total = loss_acc[phase]
        for idx in range(3):
            total = total + loss_recv[phase, idx]
        return total

    loss_acc[0] = loss_in[...]
    loss_start(0)

    low, high, every = pl.ds(0, 2), pl.ds(2, 2), pl.ds(0, 4)

    def shifted(axis, shift):
        return lax.rem(pos[axis] + shift, RING)

    def where_of(chunk, sel):
        return (chunk,) + tuple(sel[axis] for axis in 'zyx')

    def add_into(chunk, sel, buf, prefix, lead):
        free = [axis for axis in 'zyx' if axis in lead]
        start, count = lead[free[0]]

        def body(idx, carry):
            point = dict(sel)
            point[free[0]] = start + idx
            if len(free) > 1:
                point[free[1]] = every
            dst = where_of(chunk, point)
            part[dst] = part[dst] + buf[prefix[:-1] + (prefix[-1] + idx,)]
            return carry
        lax.fori_loop(0, count, body, 0)

    class Stream:
        def __init__(self, slot, first, second, base):
            self.first, self.second, self.base = first, second, base
            self.rest = GROUP_AXIS[slot]
            self.split, self.other = [axis for axis in 'zyx' if axis != first]

        def phase_copies(self, chunk, phase, kind):
            axis = (self.first, self.second)[phase]
            wide, narrow = ((r1, r2), (r3, r4))[phase]
            send, recv = (((s1_send, s1_recv), (s2_send, s2_recv)), ((s3_send, s3_recv), (s4_send, s4_recv)))[phase][kind == 2]
            copies = []
            for side in range(2):
                half = (low, high)[side ^ (kind == 1)]
                to_axis = shifted(axis, 2 if kind == 0 else (1, 3)[side])
                if phase == 0:
                    sel = {axis: to_axis, self.split: half, self.other: every}
                else:
                    sel = {self.first: pos[self.first], axis: to_axis, self.rest: half}
                dst = narrow.at[chunk, side] if kind == 2 else wide.at[chunk, side, (low, high)[kind]]
                sem_idx = (chunk, side) if kind == 2 else (chunk, side, kind)
                copies.append(remote(part.at[where_of(chunk, sel)], dst, axis, (1, 3)[side], send.at[sem_idx], recv.at[sem_idx]))
            return copies

        def exchange(self, chunk):
            g = self.rest
            copies = []
            for shift in (1, 2, 3):
                sel = {self.first: pos[self.first], self.second: pos[self.second], g: shifted(g, shift)}
                copies.append(remote(part.at[where_of(chunk, sel)], out.at[chunk, pos[g]], g, shift,
                                     a_send.at[chunk, shift - 1], a_recv.at[chunk, shift - 1]))
            return copies

        def fixed(self, phase):
            return {self.first: pos[self.first], self.second: pos[self.second]} if phase else {self.first: pos[self.first]}

        def span(self, phase, start):
            return {self.rest: (start, 2)} if phase else {self.split: (start, 2), self.other: (0, 4)}

        def send_first(self, chunk, phase):
            for kind in (0, 1):
                for copy in self.phase_copies(chunk, phase, kind):
                    copy.start()

        def send_combined(self, chunk, phase):
            relay, direct, combined = [self.phase_copies(chunk, phase, kind) for kind in range(3)]
            axis = (self.first, self.second)[phase]
            buf = (r1, r3)[phase]
            for side, (shift, start) in enumerate(((1, 0), (3, 2))):
                relay[side].wait_recv()
                sel = {**self.fixed(phase), axis: shifted(axis, shift)}
                add_into(chunk, sel, buf, (chunk, side, 0), self.span(phase, start))
                combined[side].start()
            for side, start in ((0, 2), (1, 0)):
                direct[side].wait_recv()
                add_into(chunk, self.fixed(phase), buf, (chunk, side, 2), self.span(phase, start))

        def take_combined(self, chunk, phase):
            combined = self.phase_copies(chunk, phase, 2)
            for side, start in ((0, 0), (1, 2)):
                combined[side].wait_recv()
                add_into(chunk, self.fixed(phase), (r2, r4)[phase], (chunk, side, 0), self.span(phase, start))

        def step(self, number, chunk):
            if number == 0:
                self.send_first(chunk, 0)
            elif number == 1:
                self.send_combined(chunk, 0)
            elif number == 2:
                self.take_combined(chunk, 0)
                self.send_first(chunk, 1)
            elif number == 3:
                self.send_combined(chunk, 1)
            elif number == 4:
                self.take_combined(chunk, 1)
                for copy in self.exchange(chunk):
                    copy.start()
                g = self.rest
                out[chunk, pos[g]] = part[where_of(chunk, {**self.fixed(1), g: pos[g]})]
            else:
                for copy in self.exchange(chunk):
                    copy.wait()
                for phase in range(2):
                    for kind in range(3):
                        for copy in self.phase_copies(chunk, phase, kind):
                            copy.wait_send()

    streams = {slot: [Stream(slot, OUTER[slot], 'z', slot * 8), Stream(slot, 'z', OUTER[slot], slot * 8 + 4)] for slot in (0, 1)}

    def reduce_step(number, wave, which=(0, 1)):
        slot, half = WAVES[wave]

        def body(idx, carry):
            for stream_idx in which:
                stream = streams[slot][stream_idx]
                stream.step(number, stream.base + 2 * half + idx)
            return carry
        lax.fori_loop(0, 2, body, 0)

    def hidden_step(wave):
        slot, _ = WAVES[wave]
        for copy in weight_copies(wave):
            copy.wait()

        def body(block, carry):
            pre_act = jnp.dot(gh[slot, block], one[wave % 2], preferred_element_type=jnp.float32).astype(jnp.bfloat16)
            grad_act = lax.dot_general(ge[slot, block], two[wave % 2], CONTRACT_LAST, preferred_element_type=jnp.float32).astype(jnp.bfloat16)
            value, slope = gelu_parts(pre_act.astype(jnp.float32))
            act[block] = value.astype(jnp.bfloat16)
            grad[block] = (grad_act.astype(jnp.float32) * slope).astype(jnp.bfloat16)
            return carry
        lax.fori_loop(0, RING, body, 0)
        if wave + 2 < len(WAVES):
            for copy in weight_copies(wave + 2):
                copy.start()

    def product_step(wave):
        slot, half = WAVES[wave]
        for kind, (left, right) in enumerate(((gh, grad), (ge, act))):
            first_chunk = slot * 8 + kind * 4 + 2 * half

            def body(block, carry):
                cols = pl.ds(pl.multiple_of(block * 512, 512), 512)
                lhs = left[slot, :, :, cols].reshape(RING * n_rows, 512)
                total = lax.dot_general(lhs, right[...].reshape(RING * n_rows, HIDDEN), CONTRACT_FIRST, preferred_element_type=jnp.float32)
                for piece in range(2):
                    part[first_chunk + piece, pl.ds(2 * block, 2)] = total[:, piece * COLS:(piece + 1) * COLS].reshape(2, RING, RING, 16, COLS)
                return carry
            lax.fori_loop(0, 2, body, 0)
            reduce_step(0, wave, (kind,))

    for copy in fills[1]:
        copy.wait()
    hidden_step(0)
    for copy, relay in zip(directs, e_relays()):
        copy.wait_recv()
        relay.start()
    product_step(0)
    loss_acc[1] = loss_finish(0)
    loss_start(1)
    hidden_step(1)
    reduce_step(1, 0)
    product_step(1)
    reduce_step(2, 0)
    loss_acc[2] = loss_finish(1)
    loss_start(2)
    for copy in fills[0] + [relay_done for relay_done in e_relays()]:
        copy.wait()
    for copy in directs:
        copy.wait_send()
    hidden_step(2)
    reduce_step(1, 1)
    reduce_step(3, 0)
    product_step(2)
    reduce_step(2, 1)
    reduce_step(4, 0)
    hidden_step(3)
    reduce_step(1, 2)
    reduce_step(3, 1)
    product_step(3)
    for number, wave in ((2, 2), (4, 1), (1, 3), (3, 2), (2, 3), (4, 2), (3, 3), (4, 3)):
        reduce_step(number, wave)
    loss_out[...] = loss_finish(2)
    for wave in range(len(WAVES)):
        reduce_step(5, wave)


def weight_sums(gh0, gh1, ge1, e0, w_up, w_down, loss_part):
    n_rows, n_width = e0.shape
    block = n_width // (RING * RING * RING)
    f32, bf16 = jnp.float32, jnp.bfloat16
    dma = pltpu.SemaphoreType.DMA
    vmem = pl.BlockSpec(memory_space=pltpu.VMEM)
    hbm = pl.BlockSpec(memory_space=pl.ANY)
    n_waves = len(WAVES)
    return pl.pallas_call(
        weight_kernel,
        out_shape=(jax.ShapeDtypeStruct((N_CHUNKS, RING, block, COLS), f32), jax.ShapeDtypeStruct(loss_part.shape, f32)),
        in_specs=[hbm] * 6 + [vmem],
        out_specs=(vmem, vmem),
        scratch_shapes=[
            pltpu.VMEM((2, RING, n_rows, n_width), bf16),
            pltpu.VMEM((2, RING, n_rows, n_width), bf16),
            pltpu.VMEM((2, n_width, HIDDEN), bf16),
            pltpu.VMEM((2, HIDDEN, n_width), bf16),
            pltpu.VMEM((RING, n_rows, HIDDEN), bf16),
            pltpu.VMEM((RING, n_rows, HIDDEN), bf16),
            pltpu.VMEM((N_CHUNKS, RING, RING, RING, block, COLS), f32),
            pltpu.VMEM((N_CHUNKS, 2, 4, 4, block, COLS), f32),
            pltpu.VMEM((N_CHUNKS, 2, 2, 4, block, COLS), f32),
            pltpu.VMEM((N_CHUNKS, 2, 4, block, COLS), f32),
            pltpu.VMEM((N_CHUNKS, 2, 2, block, COLS), f32),
            pltpu.VMEM((3,) + loss_part.shape, f32),
            pltpu.VMEM((3, 3) + loss_part.shape, f32),
            dma((2,)), dma((2,)), dma((n_waves,)), dma((n_waves,)), dma((4,)), dma((4,)),
            dma((N_CHUNKS, 2, 2)), dma((N_CHUNKS, 2, 2)),
            dma((N_CHUNKS, 2)), dma((N_CHUNKS, 2)),
            dma((N_CHUNKS, 2, 2)), dma((N_CHUNKS, 2, 2)),
            dma((N_CHUNKS, 2)), dma((N_CHUNKS, 2)),
            dma((N_CHUNKS, 3)), dma((N_CHUNKS, 3)),
            dma((3, 3)), dma((3, 3)),
        ],
        compiler_params=pltpu.CompilerParams(collective_id=1, has_side_effects=True, vmem_limit_bytes=67043328),
        name='weight_sums',
    )(gh0, gh1, ge1, e0, w_up, w_down, loss_part)


def chain_kernel(total_tokens, x_ref, y_ref, w_one, w_two, gh0, gh1, ge1, e0, loss_out,
                 one, two, pre, acc, h0, h1, e1, h_top, h_recv, e_recv, loss_val,
                 one_sem, two_sem, send_sem, recv_sem, own_sem, ring_send, ring_recv):
    stage_idx = lax.axis_index('stage')
    data_idx = lax.axis_index('data')
    n_layers, n_parts = one.shape[:2]
    is_first = stage_idx == 0
    is_last = stage_idx == 1

    def weight_copies(layer, part_idx):
        span = pl.ds(part_idx * HIDDEN, HIDDEN)
        return (
            pltpu.make_async_copy(w_one.at[layer, :, span], one.at[layer, part_idx], one_sem.at[layer, part_idx]),
            pltpu.make_async_copy(w_two.at[layer, span, :], two.at[layer, part_idx], two_sem.at[layer, part_idx]),
        )

    for layer in range(n_layers):
        for part_idx in range(n_parts):
            for copy in weight_copies(layer, part_idx):
                copy.start()

    barrier = pltpu.get_barrier_semaphore()
    pl.semaphore_signal(barrier, inc=1, device_id=(1 - stage_idx, data_idx), device_id_type=MESH)
    for axis in GROUP_AXIS:
        for shift in (1, 3):
            pl.semaphore_signal(barrier, inc=1, device_id=(stage_idx, neighbour(data_idx, axis, shift)), device_id_type=MESH)
    pl.semaphore_wait(barrier, 5)

    half = x_ref.shape[0] // 2
    rows = (pl.ds(0, half), pl.ds(half, half))

    def ring_copies(number):
        src, dst, axis = ((h0, gh0, 'x'), (h1, gh1, 'y'), (e1, ge1, 'y'))[number]
        here = position(data_idx, axis)

        def remote(source, target, shift, idx):
            return pltpu.make_async_remote_copy(
                src_ref=source, dst_ref=target, send_sem=ring_send.at[number, idx], recv_sem=ring_recv.at[number, idx],
                device_id=(stage_idx, neighbour(data_idx, axis, shift)), device_id_type=MESH)
        own = pltpu.make_async_copy(src, dst.at[here], own_sem.at[number])
        direct = [remote(src, dst.at[here], (1, 3)[side], side) for side in range(2)]
        relay = []
        for side, shift in ((0, 1), (1, 3)):
            block = dst.at[lax.rem(here + RING - shift, RING), rows[side]]
            relay.append(remote(block, block, shift, 2 + side))
        return own, direct, relay

    def ring_start(number):
        own, direct, _ = ring_copies(number)
        for copy in [own] + direct:
            copy.start()

    def ring_relay(number):
        _, direct, relay = ring_copies(number)
        for copy, onward in zip(direct, relay):
            copy.wait_recv()
            onward.start()

    def ring_finish(number):
        own, direct, relay = ring_copies(number)
        own.wait()
        for copy in direct:
            copy.wait_send()
        for copy in relay:
            copy.wait()

    def to_partner(src, dst, slot):
        return pltpu.make_async_remote_copy(
            src_ref=src, dst_ref=dst, send_sem=send_sem.at[slot], recv_sem=recv_sem.at[slot],
            device_id=(1 - stage_idx, data_idx), device_id_type=MESH)

    def forward(layer, src, dst):
        def body(part_idx, carry):
            for copy in weight_copies(layer, part_idx):
                copy.wait()
            pre_act = jnp.dot(src[...], one[layer, part_idx], preferred_element_type=jnp.float32).astype(jnp.bfloat16)
            pre[layer, part_idx] = pre_act
            act = gelu_parts(pre_act.astype(jnp.float32))[0].astype(jnp.bfloat16)
            acc[...] += jnp.dot(act, two[layer, part_idx], preferred_element_type=jnp.float32)
            return carry
        acc[...] = jnp.zeros_like(acc)
        lax.fori_loop(0, n_parts, body, 0)
        dst[...] = (src[...].astype(jnp.float32) + acc[...]).astype(jnp.bfloat16)

    def backward(layer, src, dst):
        def body(part_idx, carry):
            grad_act = lax.dot_general(src[...], two[layer, part_idx], CONTRACT_LAST, preferred_element_type=jnp.float32).astype(jnp.bfloat16)
            slope = gelu_parts(pre[layer, part_idx].astype(jnp.float32))[1]
            grad_pre = (grad_act.astype(jnp.float32) * slope).astype(jnp.bfloat16)
            acc[...] += lax.dot_general(grad_pre, one[layer, part_idx], CONTRACT_LAST, preferred_element_type=jnp.float32)
            return carry
        acc[...] = jnp.zeros_like(acc)
        lax.fori_loop(0, n_parts, body, 0)
        dst[...] = (src[...].astype(jnp.float32) + acc[...]).astype(jnp.bfloat16)

    @pl.when(is_first)
    def _():
        h0[...] = x_ref[...]

    @pl.when(is_last)
    def _():
        to_partner(h_top, h_recv, 0).wait_recv()
        h0[...] = h_recv[...]

    ring_start(0)
    forward(0, h0, h1)
    ring_start(1)
    ring_relay(0)
    forward(1, h1, h_top)

    @pl.when(is_first)
    def _():
        to_partner(h_top, h_recv, 0).start()
        ring_relay(1)
        to_partner(e_recv, e_recv, 1).wait_recv()
        to_partner(loss_val, loss_out, 2).wait_recv()
        e1[...] = e_recv[...]

    @pl.when(is_last)
    def _():
        diff = h_top[...].astype(jnp.float32) - y_ref[...].astype(jnp.float32)
        e1[...] = (diff / total_tokens).astype(jnp.bfloat16)
        loss_val[...] = jnp.full(loss_val.shape, jnp.sum(diff * diff) / (2 * total_tokens), jnp.float32)
        to_partner(loss_val, loss_out, 2).start()
        ring_relay(1)

    ring_start(2)
    backward(1, e1, e0)
    ring_relay(2)

    @pl.when(is_first)
    def _():
        to_partner(h_top, h_recv, 0).wait_send()

    @pl.when(is_last)
    def _():
        backward(0, e0, h_top)
        to_partner(h_top, e_recv, 1).start()
        loss_out[...] = loss_val[...]
        to_partner(h_top, e_recv, 1).wait_send()
        to_partner(loss_val, loss_out, 2).wait_send()

    for number in range(3):
        ring_finish(number)


def layer_chain(x_all, y_all, w_up, w_down, total_tokens):
    n_layers, n_width, n_ffn = w_up.shape
    n_parts = n_ffn // HIDDEN
    act = jax.ShapeDtypeStruct(x_all.shape, jnp.bfloat16)
    group = jax.ShapeDtypeStruct((RING,) + x_all.shape, jnp.bfloat16)
    vmem = pl.BlockSpec(memory_space=pltpu.VMEM)
    hbm = pl.BlockSpec(memory_space=pl.ANY)
    bf16 = jnp.bfloat16
    dma = pltpu.SemaphoreType.DMA
    return pl.pallas_call(
        functools.partial(chain_kernel, total_tokens),
        out_shape=(group, group, group, act, jax.ShapeDtypeStruct((8, 128), jnp.float32)),
        in_specs=[vmem, vmem, hbm, hbm],
        out_specs=(hbm, hbm, hbm, vmem, vmem),
        scratch_shapes=[
            pltpu.VMEM((n_layers, n_parts, n_width, HIDDEN), bf16),
            pltpu.VMEM((n_layers, n_parts, HIDDEN, n_width), bf16),
            pltpu.VMEM((n_layers, n_parts, x_all.shape[0], HIDDEN), bf16),
            pltpu.VMEM(x_all.shape, jnp.float32),
            pltpu.VMEM(x_all.shape, bf16),
            pltpu.VMEM(x_all.shape, bf16),
            pltpu.VMEM(x_all.shape, bf16),
            pltpu.VMEM(x_all.shape, bf16),
            pltpu.VMEM(x_all.shape, bf16),
            pltpu.VMEM(x_all.shape, bf16),
            pltpu.VMEM((8, 128), jnp.float32),
            dma((n_layers, n_parts)), dma((n_layers, n_parts)), dma((3,)), dma((3,)),
            dma((3,)), dma((3, 4)), dma((3, 4)),
        ],
        compiler_params=pltpu.CompilerParams(collective_id=2, has_side_effects=True, vmem_limit_bytes=62 * 1024 * 1024),
        name='layer_chain',
    )(x_all, y_all, w_up, w_down)


def solution(mesh):
    replicas = mesh.shape['data']

    def per_device(x_loc, y_loc, w_up, w_down):
        n_micro, n_tokens, n_width = x_loc.shape
        n_ffn = w_up.shape[2]
        total_tokens = replicas * n_micro * n_tokens
        x_all = x_loc.reshape(n_micro * n_tokens, n_width)
        y_all = y_loc.reshape(n_micro * n_tokens, n_width)

        gh0, gh1, ge1, e0, loss_part = layer_chain(x_all, y_all, w_up, w_down, total_tokens)
        sums, loss_sum = weight_sums(gh0, gh1, ge1, e0, w_up, w_down, loss_part)
        block = sums.shape[2]
        sums = sums.reshape(2, 2, n_ffn // RING // COLS, RING, block, COLS)
        grad_up = sums[:, 0].transpose(0, 3, 2, 1, 4).reshape(2, block, n_ffn)
        grad_down = sums[:, 1].transpose(0, 2, 1, 4, 3).reshape(2, n_ffn, block)
        return loss_sum[0, 0], grad_up, grad_down

    return jax.shard_map(
        per_device,
        mesh=mesh,
        in_specs=(P('data', None, None), P('data', None, None), P('stage', None, None), P('stage', None, None)),
        out_specs=(P(), P('stage', 'data', None), P('stage', None, 'data')),
        check_vma=False,
    )
```

```python
import functools

import jax
import jax.numpy as jnp
from jax import lax
from jax.experimental import pallas as pl
from jax.experimental.pallas import tpu as pltpu
from jax.sharding import PartitionSpec as P

CONTRACT_LAST = (((1,), (1,)), ((), ()))
CONTRACT_FIRST = (((0,), (0,)), ((), ()))
MESH = pl.DeviceIdType.MESH
RING = 4
STRIDE = {'x': 1, 'y': 4, 'z': 16}
GROUP_AXIS = ('x', 'y')
COLS = 256
HIDDEN = 512
N_CHUNKS = 16
ROOT = (2.0 / 3.141592653589793) ** 0.5
CUBIC = 0.044715


WAVES = ((1, 0), (1, 1), (0, 0), (0, 1))
OUTER = ('y', 'x')


def position(data_idx, axis):
    return lax.rem(lax.div(data_idx, STRIDE[axis]), RING)


def neighbour(data_idx, axis, shift):
    here = position(data_idx, axis)
    return data_idx + (lax.rem(here + shift, RING) - here) * STRIDE[axis]


def meet(stage_idx, data_idx, peers):
    barrier = pltpu.get_barrier_semaphore()
    for axis, shift in peers:
        pl.semaphore_signal(barrier, inc=1, device_id=(stage_idx, neighbour(data_idx, axis, shift)), device_id_type=MESH)
    pl.semaphore_wait(barrier, len(peers))


def gelu_parts(x):
    square = x * x
    tanh = jnp.tanh(x * (ROOT + (ROOT * CUBIC) * square))
    cdf = 0.5 + 0.5 * tanh
    slope = cdf + (0.5 * x) * ((1.0 - tanh * tanh) * (ROOT + (3.0 * ROOT * CUBIC) * square))
    return x * cdf, slope


def weight_kernel(gh0, gh1, ge1, e0, w_one, w_two, loss_in, out_up, out_down, loss_out,
                  gh, ge, one, two, act, grad, part, r1, r2, r3, r4, loss_acc, loss_recv,
                  gh_sem, ge_sem, one_sem, two_sem, e_send, e_recv,
                  s1_send, s1_recv, s2_send, s2_recv, s3_send, s3_recv, s4_send, s4_recv, a_send, a_recv,
                  loss_send, loss_got):
    stage_idx = lax.axis_index('stage')
    data_idx = lax.axis_index('data')
    pos = {axis: position(data_idx, axis) for axis in 'xyz'}
    n_rows = gh.shape[2]
    n_cols = w_one.shape[2] // RING

    def remote(src, dst, axis, shift, send, recv):
        return pltpu.make_async_remote_copy(
            src_ref=src, dst_ref=dst, send_sem=send, recv_sem=recv,
            device_id=(stage_idx, neighbour(data_idx, axis, shift)), device_id_type=MESH)

    def weight_copies(wave):
        slot, half = WAVES[wave]
        span = pl.ds(pl.multiple_of(pos[GROUP_AXIS[slot]] * n_cols + half * HIDDEN, HIDDEN), HIDDEN)
        return (
            pltpu.make_async_copy(w_one.at[slot, :, span], one.at[wave % 2], one_sem.at[wave]),
            pltpu.make_async_copy(w_two.at[slot, span, :], two.at[wave % 2], two_sem.at[wave]),
        )

    own_e = pltpu.make_async_copy(e0, ge.at[0, pos['x']], ge_sem.at[0, 0])
    own_e.start()

    def fills(slot, block):
        copies = [pltpu.make_async_copy((gh0, gh1)[slot].at[block], gh.at[slot, block], gh_sem.at[slot, block])]
        if slot == 1:
            copies.append(pltpu.make_async_copy(ge1.at[block], ge.at[1, block], ge_sem.at[1, block]))
        return copies

    for copy in list(weight_copies(0)) + fills(1, 0) + fills(1, 1):
        copy.start()
    meet(stage_idx, data_idx, [(axis, shift) for axis in 'xyz' for shift in (1, 2, 3)])

    here = pos['x']
    rows = (pl.ds(0, n_rows // 2), pl.ds(n_rows // 2, n_rows // 2))
    own_e.wait()

    def e_copies():
        first, later, relay = [], [], []
        for side, shift in ((0, 1), (1, 3)):
            for order, copies in ((0, first), (1, later)):
                block = ge.at[0, here, rows[side ^ order]]
                copies.append(remote(block, block, 'x', shift, e_send.at[side, order], e_recv.at[side, order]))
            block = ge.at[0, lax.rem(here + RING - shift, RING), rows[side]]
            relay.append(remote(block, block, 'x', shift, e_send.at[side, 2], e_recv.at[side, 2]))
        return first, later, relay

    for copies in e_copies()[:2]:
        for copy in copies:
            copy.start()

    def e_relay():
        first, _, relay = e_copies()
        for copy, onward in zip(first, relay):
            copy.wait_recv()
            onward.start()

    def e_finish():
        first, later, relay = e_copies()
        for copy in first:
            copy.wait_send()
        for copy in later + relay:
            copy.wait()

    def loss_copies(phase):
        return [remote(loss_acc.at[phase], loss_recv.at[phase, shift - 1], 'xyz'[phase], shift,
                       loss_send.at[phase, shift - 1], loss_got.at[phase, shift - 1]) for shift in (1, 2, 3)]

    def loss_start(phase):
        for copy in loss_copies(phase):
            copy.start()

    def loss_finish(phase):
        for copy in loss_copies(phase):
            copy.wait()
        total = loss_acc[phase]
        for idx in range(3):
            total = total + loss_recv[phase, idx]
        return total

    loss_acc[0] = loss_in[...]
    loss_start(0)

    low, high, every = pl.ds(0, 2), pl.ds(2, 2), pl.ds(0, 4)

    def shifted(axis, shift):
        return lax.rem(pos[axis] + shift, RING)

    def where_of(chunk, sel):
        return (chunk,) + tuple(sel[axis] for axis in 'zyx')

    def add_into(chunk, sel, buf, prefix, lead):
        free = [axis for axis in 'zyx' if axis in lead]
        start, count = lead[free[0]]

        def body(idx, carry):
            point = dict(sel)
            point[free[0]] = start + idx
            if len(free) > 1:
                point[free[1]] = every
            dst = where_of(chunk, point)
            part[dst] = part[dst] + buf[prefix[:-1] + (prefix[-1] + idx,)]
            return carry
        lax.fori_loop(0, count, body, 0)

    class Stream:
        def __init__(self, slot, first, second):
            self.slot, self.first, self.second = slot, first, second
            self.rest = GROUP_AXIS[slot]
            self.split, self.other = [axis for axis in 'zyx' if axis != first]

        def phase_copies(self, chunk, phase, kind):
            axis = (self.first, self.second)[phase]
            wide, narrow = ((r1, r2), (r3, r4))[phase]
            send, recv = (((s1_send, s1_recv), (s2_send, s2_recv)), ((s3_send, s3_recv), (s4_send, s4_recv)))[phase][kind == 2]
            copies = []
            for side in range(2):
                half = (low, high)[side ^ (kind == 1)]
                to_axis = shifted(axis, 2 if kind == 0 else (1, 3)[side])
                if phase == 0:
                    sel = {axis: to_axis, self.split: half, self.other: every}
                else:
                    sel = {self.first: pos[self.first], axis: to_axis, self.rest: half}
                dst = narrow.at[chunk, side] if kind == 2 else wide.at[chunk, side, (low, high)[kind]]
                sem_idx = (chunk, side) if kind == 2 else (chunk, side, kind)
                copies.append(remote(part.at[where_of(chunk, sel)], dst, axis, (1, 3)[side], send.at[sem_idx], recv.at[sem_idx]))
            return copies

        def landing(self, chunk, kind, origin):
            piece = chunk - self.slot * 8 - kind * 4
            if kind == 1:
                return out_down.at[self.slot * 4 + piece, origin]
            start = pl.multiple_of(origin * n_cols + piece * COLS, COLS)
            return out_up.at[self.slot, :, pl.ds(start, COLS)]

        def exchange(self, chunk, kind):
            g = self.rest
            copies = []
            for shift in (1, 2, 3):
                sel = {self.first: pos[self.first], self.second: pos[self.second], g: shifted(g, shift)}
                copies.append(remote(part.at[where_of(chunk, sel)], self.landing(chunk, kind, pos[g]), g, shift,
                                     a_send.at[chunk, shift - 1], a_recv.at[chunk, shift - 1]))
            return copies

        def fixed(self, phase):
            return {self.first: pos[self.first], self.second: pos[self.second]} if phase else {self.first: pos[self.first]}

        def span(self, phase, start):
            return {self.rest: (start, 2)} if phase else {self.split: (start, 2), self.other: (0, 4)}

        def send_first(self, chunk, phase):
            for kind in (0, 1):
                for copy in self.phase_copies(chunk, phase, kind):
                    copy.start()

        def send_combined(self, chunk, phase):
            relay, direct, combined = [self.phase_copies(chunk, phase, kind) for kind in range(3)]
            axis = (self.first, self.second)[phase]
            buf = (r1, r3)[phase]
            for side, (shift, start) in enumerate(((1, 0), (3, 2))):
                relay[side].wait_recv()
                sel = {**self.fixed(phase), axis: shifted(axis, shift)}
                add_into(chunk, sel, buf, (chunk, side, 0), self.span(phase, start))
                combined[side].start()
            for side, start in ((0, 2), (1, 0)):
                direct[side].wait_recv()
                add_into(chunk, self.fixed(phase), buf, (chunk, side, 2), self.span(phase, start))

        def take_combined(self, chunk, phase):
            combined = self.phase_copies(chunk, phase, 2)
            for side, start in ((0, 0), (1, 2)):
                combined[side].wait_recv()
                add_into(chunk, self.fixed(phase), (r2, r4)[phase], (chunk, side, 0), self.span(phase, start))

        def step(self, number, chunk, kind):
            if number == 0:
                self.send_first(chunk, 0)
            elif number == 1:
                self.send_combined(chunk, 0)
            elif number == 2:
                self.take_combined(chunk, 0)
                self.send_first(chunk, 1)
            elif number == 3:
                self.send_combined(chunk, 1)
            elif number == 4:
                self.take_combined(chunk, 1)
                for copy in self.exchange(chunk, kind):
                    copy.start()
                g = self.rest
                self.landing(chunk, kind, pos[g])[...] = part[where_of(chunk, {**self.fixed(1), g: pos[g]})]
            else:
                for copy in self.exchange(chunk, kind):
                    copy.wait()
                for phase in range(2):
                    for kind in range(3):
                        for copy in self.phase_copies(chunk, phase, kind):
                            copy.wait_send()

    outer_first = [Stream(slot, OUTER[slot], 'z') for slot in (0, 1)]
    depth_first = [Stream(slot, 'z', OUTER[slot]) for slot in (0, 1)]

    def reduce_step(number, wave, kinds=(0, 1)):
        slot, half = WAVES[wave]
        for kind in kinds:
            by_depth = half == 0 if slot == 1 else (half == 1 and kind == 1)
            stream = (depth_first if by_depth else outer_first)[slot]

            def body(idx, carry):
                stream.step(number, slot * 8 + kind * 4 + 2 * half + idx, kind)
                return carry
            lax.fori_loop(0, 2, body, 0)

    def hidden_step(wave):
        slot, _ = WAVES[wave]
        for copy in weight_copies(wave):
            copy.wait()

        def body(block, carry):
            if wave in (0, 2):
                for copy in fills(slot, block):
                    copy.wait()
            if wave == 0:
                @pl.when(block + 2 < RING)
                def _():
                    for copy in fills(slot, block + 2):
                        copy.start()
            pre_act = jnp.dot(gh[slot, block], one[wave % 2], preferred_element_type=jnp.float32).astype(jnp.bfloat16)
            grad_act = lax.dot_general(ge[slot, block], two[wave % 2], CONTRACT_LAST, preferred_element_type=jnp.float32).astype(jnp.bfloat16)
            value, slope = gelu_parts(pre_act.astype(jnp.float32))
            act[block] = value.astype(jnp.bfloat16)
            grad[block] = (grad_act.astype(jnp.float32) * slope).astype(jnp.bfloat16)
            return carry
        lax.fori_loop(0, RING, body, 0)
        if wave + 2 < len(WAVES):
            for copy in weight_copies(wave + 2):
                copy.start()

    def product_step(wave):
        slot, half = WAVES[wave]
        for kind, (left, right) in enumerate(((gh, grad), (ge, act))):
            first_chunk = slot * 8 + kind * 4 + 2 * half

            def body(block, carry):
                cols = pl.ds(pl.multiple_of(block * 512, 512), 512)
                lhs = left[slot, :, :, cols].reshape(RING * n_rows, 512)
                total = lax.dot_general(lhs, right[...].reshape(RING * n_rows, HIDDEN), CONTRACT_FIRST, preferred_element_type=jnp.float32)
                for piece in range(2):
                    part[first_chunk + piece, pl.ds(2 * block, 2)] = total[:, piece * COLS:(piece + 1) * COLS].reshape(2, RING, RING, 16, COLS)
                return carry
            lax.fori_loop(0, 2, body, 0)
            reduce_step(0, wave, (kind,))

    hidden_step(0)
    for copy in list(weight_copies(1)) + [copy for block in range(RING) for copy in fills(0, block)]:
        copy.start()
    e_relay()
    product_step(0)
    hidden_step(1)
    product_step(1)
    loss_acc[1] = loss_finish(0)
    loss_start(1)
    reduce_step(1, 0)
    e_finish()
    hidden_step(2)
    product_step(2)
    reduce_step(2, 0)
    loss_acc[2] = loss_finish(1)
    loss_start(2)
    hidden_step(3)
    product_step(3)
    for number, wave in ((1, 1), (3, 0), (1, 2), (2, 1), (4, 0), (2, 2), (1, 3), (3, 1), (2, 3), (3, 2), (4, 1), (3, 3), (4, 2), (4, 3)):
        reduce_step(number, wave)
    loss_out[...] = loss_finish(2)
    for wave in range(len(WAVES)):
        reduce_step(5, wave)


def weight_sums(gh0, gh1, ge1, e0, w_up, w_down, loss_part):
    n_rows, n_width = e0.shape
    block = n_width // (RING * RING * RING)
    f32, bf16 = jnp.float32, jnp.bfloat16
    dma = pltpu.SemaphoreType.DMA
    vmem = pl.BlockSpec(memory_space=pltpu.VMEM)
    hbm = pl.BlockSpec(memory_space=pl.ANY)
    n_waves = len(WAVES)
    return pl.pallas_call(
        weight_kernel,
        out_shape=(jax.ShapeDtypeStruct((2, block, w_up.shape[2]), f32), jax.ShapeDtypeStruct((N_CHUNKS // 2, RING, block, COLS), f32),
                   jax.ShapeDtypeStruct(loss_part.shape, f32)),
        in_specs=[hbm] * 6 + [vmem],
        out_specs=(vmem, vmem, vmem),
        scratch_shapes=[
            pltpu.VMEM((2, RING, n_rows, n_width), bf16),
            pltpu.VMEM((2, RING, n_rows, n_width), bf16),
            pltpu.VMEM((2, n_width, HIDDEN), bf16),
            pltpu.VMEM((2, HIDDEN, n_width), bf16),
            pltpu.VMEM((RING, n_rows, HIDDEN), bf16),
            pltpu.VMEM((RING, n_rows, HIDDEN), bf16),
            pltpu.VMEM((N_CHUNKS, RING, RING, RING, block, COLS), f32),
            pltpu.VMEM((N_CHUNKS, 2, 4, 4, block, COLS), f32),
            pltpu.VMEM((N_CHUNKS, 2, 2, 4, block, COLS), f32),
            pltpu.VMEM((N_CHUNKS, 2, 4, block, COLS), f32),
            pltpu.VMEM((N_CHUNKS, 2, 2, block, COLS), f32),
            pltpu.VMEM((3,) + loss_part.shape, f32),
            pltpu.VMEM((3, 3) + loss_part.shape, f32),
            dma((2, RING)), dma((2, RING)), dma((n_waves,)), dma((n_waves,)), dma((2, 3)), dma((2, 3)),
            dma((N_CHUNKS, 2, 2)), dma((N_CHUNKS, 2, 2)),
            dma((N_CHUNKS, 2)), dma((N_CHUNKS, 2)),
            dma((N_CHUNKS, 2, 2)), dma((N_CHUNKS, 2, 2)),
            dma((N_CHUNKS, 2)), dma((N_CHUNKS, 2)),
            dma((N_CHUNKS, 3)), dma((N_CHUNKS, 3)),
            dma((3, 3)), dma((3, 3)),
        ],
        compiler_params=pltpu.CompilerParams(collective_id=1, has_side_effects=True, vmem_limit_bytes=67043328),
        name='weight_sums',
    )(gh0, gh1, ge1, e0, w_up, w_down, loss_part)


def chain_kernel(total_tokens, x_hbm, y_hbm, w_one, w_two, gh0, gh1, ge1, e0, loss_out,
                 one, two, pre, acc, stash_a, stash_b, hs, es, y_ref, h_recv, e_recv, loss_val,
                 one_sem, two_sem, send_sem, recv_sem, own_sem, ring_send, ring_recv):
    stage_idx = lax.axis_index('stage')
    data_idx = lax.axis_index('data')
    n_layers, n_parts = one.shape[:2]
    stash = (stash_a, stash_b)
    is_first = stage_idx == 0
    is_last = stage_idx == 1

    def weight_copies(layer, part_idx):
        span = pl.ds(part_idx * HIDDEN, HIDDEN)
        return (
            pltpu.make_async_copy(w_one.at[layer, :, span], one.at[layer, part_idx], one_sem.at[layer, part_idx]),
            pltpu.make_async_copy(w_two.at[layer, span, :], two.at[layer, part_idx], two_sem.at[layer, part_idx]),
        )

    load_x = pltpu.make_async_copy(x_hbm, hs.at[0], own_sem.at[4])
    load_y = pltpu.make_async_copy(y_hbm, y_ref, own_sem.at[5])

    @pl.when(is_first)
    def _():
        load_x.start()

    @pl.when(is_last)
    def _():
        load_y.start()

    def weights_start(flat):
        for copy in weight_copies(lax.div(flat, n_parts), lax.rem(flat, n_parts)):
            copy.start()

    for flat in range(2):
        weights_start(jnp.int32(flat))

    barrier = pltpu.get_barrier_semaphore()
    pl.semaphore_signal(barrier, inc=1, device_id=(1 - stage_idx, data_idx), device_id_type=MESH)
    for axis in GROUP_AXIS:
        for shift in (1, 3):
            pl.semaphore_signal(barrier, inc=1, device_id=(stage_idx, neighbour(data_idx, axis, shift)), device_id_type=MESH)
    pl.semaphore_wait(barrier, 5)

    half = x_hbm.shape[0] // 2
    rows = (pl.ds(0, half), pl.ds(half, half))

    def ring_copies(number):
        src, dst, axis = ((hs.at[0], gh0, 'x'), (hs.at[1], gh1, 'y'), (es.at[2], ge1, 'y'))[number]
        here = position(data_idx, axis)

        def remote(source, target, shift, idx):
            return pltpu.make_async_remote_copy(
                src_ref=source, dst_ref=target, send_sem=ring_send.at[number, idx], recv_sem=ring_recv.at[number, idx],
                device_id=(stage_idx, neighbour(data_idx, axis, shift)), device_id_type=MESH)
        own = pltpu.make_async_copy(src, dst.at[here], own_sem.at[number])
        first, later, relay = [], [], []
        for side, shift in ((0, 1), (1, 3)):
            for order, copies in ((0, first), (1, later)):
                span = rows[side ^ order]
                copies.append(remote(src.at[span], dst.at[here, span], shift, 3 * side + order))
            block = dst.at[lax.rem(here + RING - shift, RING), rows[side]]
            relay.append(remote(block, block, shift, 3 * side + 2))
        return own, first, later, relay

    def ring_start(number):
        own, first, later, _ = ring_copies(number)
        for copy in [own] + first + later:
            copy.start()

    def ring_relay(number):
        _, first, _, relay = ring_copies(number)
        for copy, onward in zip(first, relay):
            copy.wait_recv()
            onward.start()

    def ring_finish(number):
        own, first, later, relay = ring_copies(number)
        own.wait()
        for copy in first:
            copy.wait_send()
        for copy in later + relay:
            copy.wait()

    def to_partner(src, dst, slot):
        return pltpu.make_async_remote_copy(
            src_ref=src, dst_ref=dst, send_sem=send_sem.at[slot], recv_sem=recv_sem.at[slot],
            device_id=(1 - stage_idx, data_idx), device_id_type=MESH)

    def pipeline(wait, produce, consume, hook=lambda step: None):
        def pair(part_idx, last):
            wait(part_idx, last)
            for idx in range(2):
                value = stash[idx][...]
                if not (last and idx == 1):
                    produce(part_idx + idx + 1, stash[1 - idx])
                consume(part_idx + idx, value)

        acc[...] = jnp.zeros_like(acc)
        wait(None, False)
        produce(0, stash[0])

        def body(step, carry):
            hook(step)
            pair(2 * step, False)
            return carry
        lax.fori_loop(0, n_parts // 2 - 1, body, 0)
        pair(n_parts - 2, True)

    def forward(layer):
        src, dst = hs.at[layer], hs.at[layer + 1]

        def wait(part_idx, last):
            if part_idx is None:
                weight_copies(layer, 0)[0].wait()

                @pl.when(layer == 0)
                def _():
                    for flat in range(2, 4):
                        weights_start(jnp.int32(flat))
                return
            flat = layer * n_parts + part_idx + 4

            @pl.when(flat < n_layers * n_parts)
            def _():
                for idx in range(2):
                    weights_start(flat + idx)
            for idx in range(2):
                if not (last and idx == 1):
                    weight_copies(layer, part_idx + idx + 1)[0].wait()
                weight_copies(layer, part_idx + idx)[1].wait()

        def produce(part_idx, buf):
            pre_act = jnp.dot(src[...], one[layer, part_idx], preferred_element_type=jnp.float32).astype(jnp.bfloat16)
            buf[...] = pre_act
            pre[layer, part_idx] = pre_act

        def consume(part_idx, pre_act):
            act = gelu_parts(pre_act.astype(jnp.float32))[0].astype(jnp.bfloat16)
            acc[...] += jnp.dot(act, two[layer, part_idx], preferred_element_type=jnp.float32)

        pipeline(wait, produce, consume)
        dst[...] = (src[...].astype(jnp.float32) + acc[...]).astype(jnp.bfloat16)

    def backward(layer):
        src, dst = es.at[layer + 1], es.at[layer]

        def produce(part_idx, buf):
            buf[...] = lax.dot_general(src[...], two[layer, part_idx], CONTRACT_LAST, preferred_element_type=jnp.float32).astype(jnp.bfloat16)

        def consume(part_idx, grad_act):
            slope = gelu_parts(pre[layer, part_idx].astype(jnp.float32))[1]
            grad_pre = (grad_act.astype(jnp.float32) * slope).astype(jnp.bfloat16)
            acc[...] += lax.dot_general(grad_pre, one[layer, part_idx], CONTRACT_LAST, preferred_element_type=jnp.float32)

        def hook(step):
            @pl.when(jnp.logical_and(step == n_parts // 2 - 2, is_first))
            def _():
                ring_relay(2)

        pipeline(lambda part_idx, last: None, produce, consume, hook)
        dst[...] = (src[...].astype(jnp.float32) + acc[...]).astype(jnp.bfloat16)

    @pl.when(is_first)
    def _():
        load_x.wait()

    @pl.when(is_last)
    def _():
        to_partner(hs.at[2], h_recv, 0).wait_recv()
        hs[0] = h_recv[...]

    def forward_body(layer, carry):
        @pl.when(layer == 0)
        def _():
            ring_start(0)

        @pl.when(layer == 1)
        def _():
            ring_start(1)
            ring_relay(0)
        forward(layer)
        return carry
    lax.fori_loop(0, n_layers, forward_body, 0)

    @pl.when(is_first)
    def _():
        to_partner(hs.at[2], h_recv, 0).start()
        ring_relay(1)
        to_partner(es.at[0], e_recv, 1).wait_recv()
        to_partner(loss_val, loss_out, 2).wait_recv()
        es[2] = e_recv[...]

    @pl.when(is_last)
    def _():
        load_y.wait()
        diff = hs[2].astype(jnp.float32) - y_ref[...].astype(jnp.float32)
        es[2] = (diff / total_tokens).astype(jnp.bfloat16)
        loss_val[...] = jnp.full(loss_val.shape, jnp.sum(diff * diff) / (2 * total_tokens), jnp.float32)
        to_partner(loss_val, loss_out, 2).start()
        ring_relay(1)

    ring_start(2)
    store = pltpu.make_async_copy(es.at[1], e0, own_sem.at[3])

    def backward_body(step, carry):
        backward(n_layers - 1 - step)

        @pl.when(step == 0)
        def _():
            store.start()

        @pl.when(jnp.logical_and(step == 0, is_last))
        def _():
            ring_relay(2)
        return carry
    lax.fori_loop(0, 1 + stage_idx, backward_body, 0)
    store.wait()

    @pl.when(is_first)
    def _():
        to_partner(hs.at[2], h_recv, 0).wait_send()

    @pl.when(is_last)
    def _():
        to_partner(es.at[0], e_recv, 1).start()
        loss_out[...] = loss_val[...]
        to_partner(es.at[0], e_recv, 1).wait_send()
        to_partner(loss_val, loss_out, 2).wait_send()

    for number in range(3):
        ring_finish(number)


def layer_chain(x_all, y_all, w_up, w_down, total_tokens):
    n_layers, n_width, n_ffn = w_up.shape
    n_parts = n_ffn // HIDDEN
    act = jax.ShapeDtypeStruct(x_all.shape, jnp.bfloat16)
    group = jax.ShapeDtypeStruct((RING,) + x_all.shape, jnp.bfloat16)
    vmem = pl.BlockSpec(memory_space=pltpu.VMEM)
    hbm = pl.BlockSpec(memory_space=pl.ANY)
    bf16 = jnp.bfloat16
    dma = pltpu.SemaphoreType.DMA
    return pl.pallas_call(
        functools.partial(chain_kernel, total_tokens),
        out_shape=(group, group, group, act, jax.ShapeDtypeStruct((8, 128), jnp.float32)),
        in_specs=[hbm, hbm, hbm, hbm],
        out_specs=(hbm, hbm, hbm, hbm, vmem),
        scratch_shapes=[
            pltpu.VMEM((n_layers, n_parts, n_width, HIDDEN), bf16),
            pltpu.VMEM((n_layers, n_parts, HIDDEN, n_width), bf16),
            pltpu.VMEM((n_layers, n_parts, x_all.shape[0], HIDDEN), bf16),
            pltpu.VMEM(x_all.shape, jnp.float32),
            pltpu.VMEM((x_all.shape[0], HIDDEN), bf16),
            pltpu.VMEM((x_all.shape[0], HIDDEN), bf16),
            pltpu.VMEM((n_layers + 1,) + x_all.shape, bf16),
            pltpu.VMEM((n_layers + 1,) + x_all.shape, bf16),
            pltpu.VMEM(x_all.shape, bf16),
            pltpu.VMEM(x_all.shape, bf16),
            pltpu.VMEM(x_all.shape, bf16),
            pltpu.VMEM((8, 128), jnp.float32),
            dma((n_layers, n_parts)), dma((n_layers, n_parts)), dma((3,)), dma((3,)),
            dma((6,)), dma((3, 6)), dma((3, 6)),
        ],
        compiler_params=pltpu.CompilerParams(collective_id=2, has_side_effects=True, vmem_limit_bytes=62 * 1024 * 1024),
        name='layer_chain',
    )(x_all, y_all, w_up, w_down)


def solution(mesh):
    replicas = mesh.shape['data']

    def per_device(x_loc, y_loc, w_up, w_down):
        n_micro, n_tokens, n_width = x_loc.shape
        n_ffn = w_up.shape[2]
        total_tokens = replicas * n_micro * n_tokens
        x_all = x_loc.reshape(n_micro * n_tokens, n_width)
        y_all = y_loc.reshape(n_micro * n_tokens, n_width)

        gh0, gh1, ge1, e0, loss_part = layer_chain(x_all, y_all, w_up, w_down, total_tokens)
        grad_up, down, loss_sum = weight_sums(gh0, gh1, ge1, e0, w_up, w_down, loss_part)
        block = down.shape[2]
        down = down.reshape(2, n_ffn // RING // COLS, RING, block, COLS)
        grad_down = down.transpose(0, 2, 1, 4, 3).reshape(2, n_ffn, block)
        return loss_sum[0, 0], grad_up, grad_down

    return jax.shard_map(
        per_device,
        mesh=mesh,
        in_specs=(P('data', None, None), P('data', None, None), P('stage', None, None), P('stage', None, None)),
        out_specs=(P(), P('stage', 'data', None), P('stage', None, 'data')),
        check_vma=False,
    )
```

```python
import functools

import jax
import jax.numpy as jnp
from jax import lax
from jax.experimental import pallas as pl
from jax.experimental.pallas import tpu as pltpu
from jax.sharding import PartitionSpec as P

CONTRACT_LAST = (((1,), (1,)), ((), ()))
CONTRACT_FIRST = (((0,), (0,)), ((), ()))
MESH = pl.DeviceIdType.MESH
RING = 4
STRIDE = {'x': 1, 'y': 4, 'z': 16}
GROUP_AXIS = ('x', 'y')
COLS = 256
HIDDEN = 512
N_CHUNKS = 16
ROOT = (2.0 / 3.141592653589793) ** 0.5
CUBIC = 0.044715


WAVES = ((1, 0), (0, 0), (1, 1), (0, 1))
OUTER = ('y', 'x')
ORDER = (
    'H1', 'P10', 'R100', 'R101', 'P11', 'H2', 'P20', 'R110', 'P21', 'R111', 'H3', 'R120',
    'R210', 'P30', 'R121', 'R200', 'R201', 'P31', 'R221', 'R211', 'R130', 'R220', 'R310', 'R300',
    'R321', 'R131', 'R230', 'R400', 'R311', 'R231', 'R301', 'R320', 'R330', 'R411', 'R410', 'R421',
    'R331', 'R430', 'R420', 'R401', 'R431',
)


def position(data_idx, axis):
    return lax.rem(lax.div(data_idx, STRIDE[axis]), RING)


def neighbour(data_idx, axis, shift):
    here = position(data_idx, axis)
    return data_idx + (lax.rem(here + shift, RING) - here) * STRIDE[axis]


def meet(stage_idx, data_idx, peers):
    barrier = pltpu.get_barrier_semaphore()
    for axis, shift in peers:
        pl.semaphore_signal(barrier, inc=1, device_id=(stage_idx, neighbour(data_idx, axis, shift)), device_id_type=MESH)
    pl.semaphore_wait(barrier, len(peers))


def gelu_parts(x):
    square = x * x
    tanh = jnp.tanh(x * (ROOT + (ROOT * CUBIC) * square))
    cdf = 0.5 + 0.5 * tanh
    slope = cdf + (0.5 * x) * ((1.0 - tanh * tanh) * (ROOT + (3.0 * ROOT * CUBIC) * square))
    return x * cdf, slope


def weight_kernel(gh0, gh1, ge1, e0, w_one, w_two, loss_in, out_up, out_down, loss_out,
                  gh, ge, one, two, act, grad, part, r1, r2, r3, r4, loss_acc, loss_recv,
                  gh_sem, ge_sem, one_sem, two_sem, e_send, e_recv,
                  s1_send, s1_recv, s2_send, s2_recv, s3_send, s3_recv, s4_send, s4_recv, a_send, a_recv,
                  loss_send, loss_got):
    stage_idx = lax.axis_index('stage')
    data_idx = lax.axis_index('data')
    pos = {axis: position(data_idx, axis) for axis in 'xyz'}
    n_rows = gh.shape[2]
    n_cols = w_one.shape[2] // RING

    def remote(src, dst, axis, shift, send, recv):
        return pltpu.make_async_remote_copy(
            src_ref=src, dst_ref=dst, send_sem=send, recv_sem=recv,
            device_id=(stage_idx, neighbour(data_idx, axis, shift)), device_id_type=MESH)

    def weight_copies(wave):
        slot, half = WAVES[wave]
        span = pl.ds(pl.multiple_of(pos[GROUP_AXIS[slot]] * n_cols + half * HIDDEN, HIDDEN), HIDDEN)
        return (
            pltpu.make_async_copy(w_one.at[slot, :, span], one.at[wave % 2], one_sem.at[wave]),
            pltpu.make_async_copy(w_two.at[slot, span, :], two.at[wave % 2], two_sem.at[wave]),
        )

    own_e = pltpu.make_async_copy(e0, ge.at[0, pos['x']], ge_sem.at[0, 0])
    own_e.start()

    def fills(slot, block):
        copies = [pltpu.make_async_copy((gh0, gh1)[slot].at[block], gh.at[slot, block], gh_sem.at[slot, block])]
        if slot == 1:
            copies.append(pltpu.make_async_copy(ge1.at[block], ge.at[1, block], ge_sem.at[1, block]))
        return copies

    for copy in list(weight_copies(0)) + fills(1, 0) + fills(1, 1):
        copy.start()
    meet(stage_idx, data_idx, [(axis, shift) for axis in 'xyz' for shift in (1, 2, 3)])

    here = pos['x']
    rows = (pl.ds(0, n_rows // 2), pl.ds(n_rows // 2, n_rows // 2))
    own_e.wait()

    def e_copies():
        first, later, relay = [], [], []
        for side, shift in ((0, 1), (1, 3)):
            for order, copies in ((0, first), (1, later)):
                block = ge.at[0, here, rows[side ^ order]]
                copies.append(remote(block, block, 'x', shift, e_send.at[side, order], e_recv.at[side, order]))
            block = ge.at[0, lax.rem(here + RING - shift, RING), rows[side]]
            relay.append(remote(block, block, 'x', shift, e_send.at[side, 2], e_recv.at[side, 2]))
        return first, later, relay

    for copies in e_copies()[:2]:
        for copy in copies:
            copy.start()

    def e_relay():
        first, _, relay = e_copies()
        for copy, onward in zip(first, relay):
            copy.wait_recv()
            onward.start()

    def e_finish():
        first, later, relay = e_copies()
        for copy in first:
            copy.wait_send()
        for copy in later + relay:
            copy.wait()

    def loss_copies(phase):
        return [remote(loss_acc.at[phase], loss_recv.at[phase, shift - 1], 'xyz'[phase], shift,
                       loss_send.at[phase, shift - 1], loss_got.at[phase, shift - 1]) for shift in (1, 2, 3)]

    def loss_start(phase):
        for copy in loss_copies(phase):
            copy.start()

    def loss_finish(phase):
        for copy in loss_copies(phase):
            copy.wait()
        total = loss_acc[phase]
        for idx in range(3):
            total = total + loss_recv[phase, idx]
        return total

    loss_acc[0] = loss_in[...]
    loss_start(0)

    low, high, every = pl.ds(0, 2), pl.ds(2, 2), pl.ds(0, 4)

    def shifted(axis, shift):
        return lax.rem(pos[axis] + shift, RING)

    def where_of(chunk, sel):
        return (chunk,) + tuple(sel[axis] for axis in 'zyx')

    def add_into(chunk, sel, buf, prefix, lead):
        free = [axis for axis in 'zyx' if axis in lead]
        start, count = lead[free[0]]

        def body(idx, carry):
            point = dict(sel)
            point[free[0]] = start + idx
            if len(free) > 1:
                point[free[1]] = every
            dst = where_of(chunk, point)
            part[dst] = part[dst] + buf[prefix[:-1] + (prefix[-1] + idx,)]
            return carry
        lax.fori_loop(0, count, body, 0)

    class Stream:
        def __init__(self, slot, first, second):
            self.slot, self.first, self.second = slot, first, second
            self.rest = GROUP_AXIS[slot]
            self.split, self.other = [axis for axis in 'zyx' if axis != first]

        def phase_copies(self, chunk, phase, kind):
            axis = (self.first, self.second)[phase]
            wide, narrow = ((r1, r2), (r3, r4))[phase]
            send, recv = (((s1_send, s1_recv), (s2_send, s2_recv)), ((s3_send, s3_recv), (s4_send, s4_recv)))[phase][kind == 2]
            copies = []
            for side in range(2):
                half = (low, high)[side ^ (kind == 1)]
                to_axis = shifted(axis, 2 if kind == 0 else (1, 3)[side])
                if phase == 0:
                    sel = {axis: to_axis, self.split: half, self.other: every}
                else:
                    sel = {self.first: pos[self.first], axis: to_axis, self.rest: half}
                dst = narrow.at[chunk, side] if kind == 2 else wide.at[chunk, side, (low, high)[kind]]
                sem_idx = (chunk, side) if kind == 2 else (chunk, side, kind)
                copies.append(remote(part.at[where_of(chunk, sel)], dst, axis, (1, 3)[side], send.at[sem_idx], recv.at[sem_idx]))
            return copies

        def landing(self, chunk, kind, origin):
            piece = chunk - self.slot * 8 - kind * 4
            if kind == 1:
                return out_down.at[self.slot * 4 + piece, origin]
            start = pl.multiple_of(origin * n_cols + piece * COLS, COLS)
            return out_up.at[self.slot, :, pl.ds(start, COLS)]

        def exchange(self, chunk, kind):
            g = self.rest
            copies = []
            for shift in (1, 2, 3):
                sel = {self.first: pos[self.first], self.second: pos[self.second], g: shifted(g, shift)}
                copies.append(remote(part.at[where_of(chunk, sel)], self.landing(chunk, kind, pos[g]), g, shift,
                                     a_send.at[chunk, shift - 1], a_recv.at[chunk, shift - 1]))
            return copies

        def fixed(self, phase):
            return {self.first: pos[self.first], self.second: pos[self.second]} if phase else {self.first: pos[self.first]}

        def span(self, phase, start):
            return {self.rest: (start, 2)} if phase else {self.split: (start, 2), self.other: (0, 4)}

        def send_first(self, chunk, phase):
            for kind in (0, 1):
                for copy in self.phase_copies(chunk, phase, kind):
                    copy.start()

        def send_combined(self, chunk, phase):
            relay, direct, combined = [self.phase_copies(chunk, phase, kind) for kind in range(3)]
            axis = (self.first, self.second)[phase]
            buf = (r1, r3)[phase]
            for side, (shift, start) in enumerate(((1, 0), (3, 2))):
                relay[side].wait_recv()
                sel = {**self.fixed(phase), axis: shifted(axis, shift)}
                add_into(chunk, sel, buf, (chunk, side, 0), self.span(phase, start))
                combined[side].start()
            for side, start in ((0, 2), (1, 0)):
                direct[side].wait_recv()
                add_into(chunk, self.fixed(phase), buf, (chunk, side, 2), self.span(phase, start))

        def take_combined(self, chunk, phase):
            combined = self.phase_copies(chunk, phase, 2)
            for side, start in ((0, 0), (1, 2)):
                combined[side].wait_recv()
                add_into(chunk, self.fixed(phase), (r2, r4)[phase], (chunk, side, 0), self.span(phase, start))

        def step(self, number, chunk, kind):
            if number == 0:
                self.send_first(chunk, 0)
            elif number == 1:
                self.send_combined(chunk, 0)
            elif number == 2:
                self.take_combined(chunk, 0)
                self.send_first(chunk, 1)
            elif number == 3:
                self.send_combined(chunk, 1)
            elif number == 4:
                self.take_combined(chunk, 1)
                for copy in self.exchange(chunk, kind):
                    copy.start()
                g = self.rest
                self.landing(chunk, kind, pos[g])[...] = part[where_of(chunk, {**self.fixed(1), g: pos[g]})]
            else:
                for copy in self.exchange(chunk, kind):
                    copy.wait()
                for phase in range(2):
                    for kind in range(3):
                        for copy in self.phase_copies(chunk, phase, kind):
                            copy.wait_send()

    outer_first = [Stream(slot, OUTER[slot], 'z') for slot in (0, 1)]
    depth_first = [Stream(slot, 'z', OUTER[slot]) for slot in (0, 1)]

    def reduce_step(number, wave, kinds=(0, 1)):
        slot, half = WAVES[wave]
        for kind in kinds:
            by_depth = half == 0 if slot == 1 else (half == 1 and kind == 0)
            stream = (depth_first if by_depth else outer_first)[slot]

            def body(idx, carry):
                stream.step(number, slot * 8 + kind * 4 + 2 * half + idx, kind)
                return carry
            lax.fori_loop(0, 2, body, 0)

    def hidden_step(wave):
        slot, _ = WAVES[wave]
        for copy in weight_copies(wave):
            copy.wait()

        def body(block, carry):
            if wave < 2:
                for copy in fills(slot, block):
                    copy.wait()
            if wave == 0:
                @pl.when(block + 2 < RING)
                def _():
                    for copy in fills(slot, block + 2):
                        copy.start()
            pre_act = jnp.dot(gh[slot, block], one[wave % 2], preferred_element_type=jnp.float32).astype(jnp.bfloat16)
            grad_act = lax.dot_general(ge[slot, block], two[wave % 2], CONTRACT_LAST, preferred_element_type=jnp.float32).astype(jnp.bfloat16)
            value, slope = gelu_parts(pre_act.astype(jnp.float32))
            act[block] = value.astype(jnp.bfloat16)
            grad[block] = (grad_act.astype(jnp.float32) * slope).astype(jnp.bfloat16)
            return carry
        lax.fori_loop(0, RING, body, 0)
        if wave + 2 < len(WAVES):
            for copy in weight_copies(wave + 2):
                copy.start()

    def product_step(wave, kinds=(0, 1)):
        slot, half = WAVES[wave]
        for kind in kinds:
            left, right = ((gh, grad), (ge, act))[kind]
            first_chunk = slot * 8 + kind * 4 + 2 * half

            def body(block, carry):
                cols = pl.ds(pl.multiple_of(block * 512, 512), 512)
                lhs = left[slot, :, :, cols].reshape(RING * n_rows, 512)
                total = lax.dot_general(lhs, right[...].reshape(RING * n_rows, HIDDEN), CONTRACT_FIRST, preferred_element_type=jnp.float32)
                for piece in range(2):
                    part[first_chunk + piece, pl.ds(2 * block, 2)] = total[:, piece * COLS:(piece + 1) * COLS].reshape(2, RING, RING, 16, COLS)
                return carry
            lax.fori_loop(0, 2, body, 0)
            reduce_step(0, wave, (kind,))

    hidden_step(0)
    for copy in list(weight_copies(1)) + [copy for block in range(RING) for copy in fills(0, block)]:
        copy.start()
    e_relay()
    product_step(0)
    loss_acc[1] = loss_finish(0)
    loss_start(1)
    e_finish()
    for entry in ORDER:
        numbers = [int(digit) for digit in entry[1:]]
        if entry[0] == 'H':
            hidden_step(*numbers)
        elif entry[0] == 'P':
            product_step(numbers[0], numbers[1:])
        else:
            reduce_step(numbers[0], numbers[1], numbers[2:])
        if entry == 'P11':
            loss_acc[2] = loss_finish(1)
            loss_start(2)
    loss_out[...] = loss_finish(2)
    for wave in range(len(WAVES)):
        reduce_step(5, wave)


def weight_sums(gh0, gh1, ge1, e0, w_up, w_down, loss_part):
    n_rows, n_width = e0.shape
    block = n_width // (RING * RING * RING)
    f32, bf16 = jnp.float32, jnp.bfloat16
    dma = pltpu.SemaphoreType.DMA
    vmem = pl.BlockSpec(memory_space=pltpu.VMEM)
    hbm = pl.BlockSpec(memory_space=pl.ANY)
    n_waves = len(WAVES)
    return pl.pallas_call(
        weight_kernel,
        out_shape=(jax.ShapeDtypeStruct((2, block, w_up.shape[2]), f32), jax.ShapeDtypeStruct((N_CHUNKS // 2, RING, block, COLS), f32),
                   jax.ShapeDtypeStruct(loss_part.shape, f32)),
        in_specs=[hbm] * 6 + [vmem],
        out_specs=(vmem, vmem, vmem),
        scratch_shapes=[
            pltpu.VMEM((2, RING, n_rows, n_width), bf16),
            pltpu.VMEM((2, RING, n_rows, n_width), bf16),
            pltpu.VMEM((2, n_width, HIDDEN), bf16),
            pltpu.VMEM((2, HIDDEN, n_width), bf16),
            pltpu.VMEM((RING, n_rows, HIDDEN), bf16),
            pltpu.VMEM((RING, n_rows, HIDDEN), bf16),
            pltpu.VMEM((N_CHUNKS, RING, RING, RING, block, COLS), f32),
            pltpu.VMEM((N_CHUNKS, 2, 4, 4, block, COLS), f32),
            pltpu.VMEM((N_CHUNKS, 2, 2, 4, block, COLS), f32),
            pltpu.VMEM((N_CHUNKS, 2, 4, block, COLS), f32),
            pltpu.VMEM((N_CHUNKS, 2, 2, block, COLS), f32),
            pltpu.VMEM((3,) + loss_part.shape, f32),
            pltpu.VMEM((3, 3) + loss_part.shape, f32),
            dma((2, RING)), dma((2, RING)), dma((n_waves,)), dma((n_waves,)), dma((2, 3)), dma((2, 3)),
            dma((N_CHUNKS, 2, 2)), dma((N_CHUNKS, 2, 2)),
            dma((N_CHUNKS, 2)), dma((N_CHUNKS, 2)),
            dma((N_CHUNKS, 2, 2)), dma((N_CHUNKS, 2, 2)),
            dma((N_CHUNKS, 2)), dma((N_CHUNKS, 2)),
            dma((N_CHUNKS, 3)), dma((N_CHUNKS, 3)),
            dma((3, 3)), dma((3, 3)),
        ],
        compiler_params=pltpu.CompilerParams(collective_id=1, has_side_effects=True, vmem_limit_bytes=67043328),
        name='weight_sums',
    )(gh0, gh1, ge1, e0, w_up, w_down, loss_part)


def chain_kernel(total_tokens, x_hbm, y_hbm, w_one, w_two, gh0, gh1, ge1, e0, loss_out,
                 one, two, pre, acc, stash_a, stash_b, hs, es, y_ref, h_recv, e_recv, loss_val,
                 one_sem, two_sem, send_sem, recv_sem, own_sem, ring_send, ring_recv):
    stage_idx = lax.axis_index('stage')
    data_idx = lax.axis_index('data')
    n_layers, n_parts = one.shape[:2]
    stash = (stash_a, stash_b)
    is_first = stage_idx == 0
    is_last = stage_idx == 1

    def weight_copies(layer, part_idx):
        span = pl.ds(part_idx * HIDDEN, HIDDEN)
        return (
            pltpu.make_async_copy(w_one.at[layer, :, span], one.at[layer, part_idx], one_sem.at[layer, part_idx]),
            pltpu.make_async_copy(w_two.at[layer, span, :], two.at[layer, part_idx], two_sem.at[layer, part_idx]),
        )

    load_x = pltpu.make_async_copy(x_hbm, hs.at[0], own_sem.at[4])
    load_y = pltpu.make_async_copy(y_hbm, y_ref, own_sem.at[5])

    @pl.when(is_first)
    def _():
        load_x.start()

    @pl.when(is_last)
    def _():
        load_y.start()

    def weights_start(flat):
        for copy in weight_copies(lax.div(flat, n_parts), lax.rem(flat, n_parts)):
            copy.start()

    for flat in range(2):
        weights_start(jnp.int32(flat))

    barrier = pltpu.get_barrier_semaphore()
    pl.semaphore_signal(barrier, inc=1, device_id=(1 - stage_idx, data_idx), device_id_type=MESH)
    for axis in GROUP_AXIS:
        for shift in (1, 3):
            pl.semaphore_signal(barrier, inc=1, device_id=(stage_idx, neighbour(data_idx, axis, shift)), device_id_type=MESH)
    pl.semaphore_wait(barrier, 5)

    half = x_hbm.shape[0] // 2
    rows = (pl.ds(0, half), pl.ds(half, half))

    def ring_copies(number):
        src, dst, axis = ((hs.at[0], gh0, 'x'), (hs.at[1], gh1, 'y'), (es.at[2], ge1, 'y'))[number]
        here = position(data_idx, axis)

        def remote(source, target, shift, idx):
            return pltpu.make_async_remote_copy(
                src_ref=source, dst_ref=target, send_sem=ring_send.at[number, idx], recv_sem=ring_recv.at[number, idx],
                device_id=(stage_idx, neighbour(data_idx, axis, shift)), device_id_type=MESH)
        own = pltpu.make_async_copy(src, dst.at[here], own_sem.at[number])
        first, later, relay = [], [], []
        for side, shift in ((0, 1), (1, 3)):
            for order, copies in ((0, first), (1, later)):
                span = rows[side ^ order]
                copies.append(remote(src.at[span], dst.at[here, span], shift, 3 * side + order))
            block = dst.at[lax.rem(here + RING - shift, RING), rows[side]]
            relay.append(remote(block, block, shift, 3 * side + 2))
        return own, first, later, relay

    def ring_start(number):
        own, first, later, _ = ring_copies(number)
        for copy in [own] + first + later:
            copy.start()

    def ring_relay(number):
        _, first, _, relay = ring_copies(number)
        for copy, onward in zip(first, relay):
            copy.wait_recv()
            onward.start()

    def ring_finish(number):
        own, first, later, relay = ring_copies(number)
        own.wait()
        for copy in first:
            copy.wait_send()
        for copy in later + relay:
            copy.wait()

    def to_partner(src, dst, slot):
        return pltpu.make_async_remote_copy(
            src_ref=src, dst_ref=dst, send_sem=send_sem.at[slot], recv_sem=recv_sem.at[slot],
            device_id=(1 - stage_idx, data_idx), device_id_type=MESH)

    def pipeline(wait, produce, consume, hook=lambda step: None):
        def pair(part_idx, last):
            wait(part_idx, last)
            for idx in range(2):
                value = stash[idx][...]
                if not (last and idx == 1):
                    produce(part_idx + idx + 1, stash[1 - idx])
                consume(part_idx + idx, value)

        acc[...] = jnp.zeros_like(acc)
        wait(None, False)
        produce(0, stash[0])

        def body(step, carry):
            hook(step)
            pair(2 * step, False)
            return carry
        lax.fori_loop(0, n_parts // 2 - 1, body, 0)
        pair(n_parts - 2, True)

    def forward(layer):
        src, dst = hs.at[layer], hs.at[layer + 1]

        def wait(part_idx, last):
            if part_idx is None:
                weight_copies(layer, 0)[0].wait()

                @pl.when(layer == 0)
                def _():
                    for flat in range(2, 4):
                        weights_start(jnp.int32(flat))
                return
            flat = layer * n_parts + part_idx + 4

            @pl.when(flat < n_layers * n_parts)
            def _():
                for idx in range(2):
                    weights_start(flat + idx)
            for idx in range(2):
                if not (last and idx == 1):
                    weight_copies(layer, part_idx + idx + 1)[0].wait()
                weight_copies(layer, part_idx + idx)[1].wait()

        def produce(part_idx, buf):
            pre_act = jnp.dot(src[...], one[layer, part_idx], preferred_element_type=jnp.float32).astype(jnp.bfloat16)
            buf[...] = pre_act
            pre[layer, part_idx] = pre_act

        def consume(part_idx, pre_act):
            act = gelu_parts(pre_act.astype(jnp.float32))[0].astype(jnp.bfloat16)
            acc[...] += jnp.dot(act, two[layer, part_idx], preferred_element_type=jnp.float32)

        pipeline(wait, produce, consume)
        dst[...] = (src[...].astype(jnp.float32) + acc[...]).astype(jnp.bfloat16)

    def backward(layer):
        src, dst = es.at[layer + 1], es.at[layer]

        def produce(part_idx, buf):
            buf[...] = lax.dot_general(src[...], two[layer, part_idx], CONTRACT_LAST, preferred_element_type=jnp.float32).astype(jnp.bfloat16)

        def consume(part_idx, grad_act):
            slope = gelu_parts(pre[layer, part_idx].astype(jnp.float32))[1]
            grad_pre = (grad_act.astype(jnp.float32) * slope).astype(jnp.bfloat16)
            acc[...] += lax.dot_general(grad_pre, one[layer, part_idx], CONTRACT_LAST, preferred_element_type=jnp.float32)

        def hook(step):
            @pl.when(jnp.logical_and(step == n_parts // 2 - 2, is_first))
            def _():
                ring_relay(2)

        pipeline(lambda part_idx, last: None, produce, consume, hook)
        dst[...] = (src[...].astype(jnp.float32) + acc[...]).astype(jnp.bfloat16)

    @pl.when(is_first)
    def _():
        load_x.wait()

    @pl.when(is_last)
    def _():
        to_partner(hs.at[2], h_recv, 0).wait_recv()
        hs[0] = h_recv[...]

    def forward_body(layer, carry):
        @pl.when(layer == 0)
        def _():
            ring_start(0)

        @pl.when(layer == 1)
        def _():
            ring_start(1)
            ring_relay(0)
        forward(layer)
        return carry
    lax.fori_loop(0, n_layers, forward_body, 0)

    @pl.when(is_first)
    def _():
        to_partner(hs.at[2], h_recv, 0).start()
        ring_relay(1)
        to_partner(es.at[0], e_recv, 1).wait_recv()
        to_partner(loss_val, loss_out, 2).wait_recv()
        es[2] = e_recv[...]

    @pl.when(is_last)
    def _():
        load_y.wait()
        diff = hs[2].astype(jnp.float32) - y_ref[...].astype(jnp.float32)
        es[2] = (diff / total_tokens).astype(jnp.bfloat16)
        loss_val[...] = jnp.full(loss_val.shape, jnp.sum(diff * diff) / (2 * total_tokens), jnp.float32)
        to_partner(loss_val, loss_out, 2).start()
        ring_relay(1)

    ring_start(2)
    store = pltpu.make_async_copy(es.at[1], e0, own_sem.at[3])

    def backward_body(step, carry):
        backward(n_layers - 1 - step)

        @pl.when(step == 0)
        def _():
            store.start()

        @pl.when(jnp.logical_and(step == 0, is_last))
        def _():
            ring_relay(2)
        return carry
    lax.fori_loop(0, 1 + stage_idx, backward_body, 0)
    store.wait()

    @pl.when(is_first)
    def _():
        to_partner(hs.at[2], h_recv, 0).wait_send()

    @pl.when(is_last)
    def _():
        to_partner(es.at[0], e_recv, 1).start()
        loss_out[...] = loss_val[...]
        to_partner(es.at[0], e_recv, 1).wait_send()
        to_partner(loss_val, loss_out, 2).wait_send()

    for number in range(3):
        ring_finish(number)


def layer_chain(x_all, y_all, w_up, w_down, total_tokens):
    n_layers, n_width, n_ffn = w_up.shape
    n_parts = n_ffn // HIDDEN
    act = jax.ShapeDtypeStruct(x_all.shape, jnp.bfloat16)
    group = jax.ShapeDtypeStruct((RING,) + x_all.shape, jnp.bfloat16)
    vmem = pl.BlockSpec(memory_space=pltpu.VMEM)
    hbm = pl.BlockSpec(memory_space=pl.ANY)
    bf16 = jnp.bfloat16
    dma = pltpu.SemaphoreType.DMA
    return pl.pallas_call(
        functools.partial(chain_kernel, total_tokens),
        out_shape=(group, group, group, act, jax.ShapeDtypeStruct((8, 128), jnp.float32)),
        in_specs=[hbm, hbm, hbm, hbm],
        out_specs=(hbm, hbm, hbm, hbm, vmem),
        scratch_shapes=[
            pltpu.VMEM((n_layers, n_parts, n_width, HIDDEN), bf16),
            pltpu.VMEM((n_layers, n_parts, HIDDEN, n_width), bf16),
            pltpu.VMEM((n_layers, n_parts, x_all.shape[0], HIDDEN), bf16),
            pltpu.VMEM(x_all.shape, jnp.float32),
            pltpu.VMEM((x_all.shape[0], HIDDEN), bf16),
            pltpu.VMEM((x_all.shape[0], HIDDEN), bf16),
            pltpu.VMEM((n_layers + 1,) + x_all.shape, bf16),
            pltpu.VMEM((n_layers + 1,) + x_all.shape, bf16),
            pltpu.VMEM(x_all.shape, bf16),
            pltpu.VMEM(x_all.shape, bf16),
            pltpu.VMEM(x_all.shape, bf16),
            pltpu.VMEM((8, 128), jnp.float32),
            dma((n_layers, n_parts)), dma((n_layers, n_parts)), dma((3,)), dma((3,)),
            dma((6,)), dma((3, 6)), dma((3, 6)),
        ],
        compiler_params=pltpu.CompilerParams(collective_id=2, has_side_effects=True, vmem_limit_bytes=62 * 1024 * 1024),
        name='layer_chain',
    )(x_all, y_all, w_up, w_down)


def solution(mesh):
    replicas = mesh.shape['data']

    def per_device(x_loc, y_loc, w_up, w_down):
        n_micro, n_tokens, n_width = x_loc.shape
        n_ffn = w_up.shape[2]
        total_tokens = replicas * n_micro * n_tokens
        x_all = x_loc.reshape(n_micro * n_tokens, n_width)
        y_all = y_loc.reshape(n_micro * n_tokens, n_width)

        gh0, gh1, ge1, e0, loss_part = layer_chain(x_all, y_all, w_up, w_down, total_tokens)
        grad_up, down, loss_sum = weight_sums(gh0, gh1, ge1, e0, w_up, w_down, loss_part)
        block = down.shape[2]
        down = down.reshape(2, n_ffn // RING // COLS, RING, block, COLS)
        grad_down = down.transpose(0, 2, 1, 4, 3).reshape(2, n_ffn, block)
        return loss_sum[0, 0], grad_up, grad_down

    return jax.shard_map(
        per_device,
        mesh=mesh,
        in_specs=(P('data', None, None), P('data', None, None), P('stage', None, None), P('stage', None, None)),
        out_specs=(P(), P('stage', 'data', None), P('stage', None, 'data')),
        check_vma=False,
    )
```
